128 devices in a mesh: tp: 2 (over core), sp: 64 (over z, y, x).
Axes of the slice: x: 4, y: 4, z: 4, core: 2. Of those that a mesh axis runs over, the one named last changes fastest.
Arguments:
- x: bfloat16 [8, 4096], replicated
- seq_len: int32 [8], replicated
- ln_w: bfloat16 [4096], replicated
- w_q: bfloat16 [4096, 4096], P(None, 'tp')
- w_o: bfloat16 [4096, 4096], P('tp')
- w_gate: bfloat16 [4096, 12288], P(None, 'tp')
- w_up: bfloat16 [4096, 12288], P(None, 'tp')
- w_down: bfloat16 [12288, 4096], P('tp')
- k_cache: bfloat16 [8, 8, 32768, 128], P(None, 'tp', 'sp')
- v_cache: bfloat16 [8, 8, 32768, 128], P(None, 'tp', 'sp')
Outputs:
- output: bfloat16 [8, 4096], replicated
All inputs are finite; a program needn't handle non-finite values.
Results may differ from the reference program's by a relative error of at most 0.00725907.
Values sent between devices are 32-bit elements.
A program may use at most 1 GiB of HBM per device.

```python
import jax
import jax.numpy as jnp
from jax import lax

BATCH_ROWS = 8
HIDDEN = 4096
Q_HEADS = 32
KV_HEADS = 8
HEAD_DIM = 128
FFN_DIM = 12288
SEQ_LEN = 32768
LN_EPS = 1e-5


def setup_inputs(seed: int = 0) -> dict:
    keys = jax.random.split(jax.random.key(seed), 10)
    q_width = Q_HEADS * HEAD_DIM
    cache_shape = (BATCH_ROWS, KV_HEADS, SEQ_LEN, HEAD_DIM)
    out_scale = (SEQ_LEN / 16.0) ** 0.5 * q_width ** -0.5

    def normal_draw(rng_key, shape, scale):
        return (jax.random.normal(rng_key, shape, jnp.float32) * scale).astype(jnp.bfloat16)

    seq_len = jax.random.randint(keys[1], (BATCH_ROWS,), SEQ_LEN // 2, SEQ_LEN, jnp.int32)
    seq_len = seq_len.at[0].set(SEQ_LEN - 1)
    ln_w = (1.0 + 0.3 * jax.random.normal(keys[2], (HIDDEN,), jnp.float32)).astype(jnp.bfloat16)
    return {
        'x': normal_draw(keys[0], (BATCH_ROWS, HIDDEN), 1.0),
        'seq_len': seq_len,
        'ln_w': ln_w,
        'w_q': normal_draw(keys[3], (HIDDEN, q_width), HIDDEN ** -0.5),
        'w_o': normal_draw(keys[4], (q_width, HIDDEN), out_scale),
        'w_gate': normal_draw(keys[5], (HIDDEN, FFN_DIM), HIDDEN ** -0.5),
        'w_up': normal_draw(keys[6], (HIDDEN, FFN_DIM), HIDDEN ** -0.5),
        'w_down': normal_draw(keys[7], (FFN_DIM, HIDDEN), FFN_DIM ** -0.5),
        'k_cache': normal_draw(keys[8], cache_shape, 1.5),
        'v_cache': normal_draw(keys[9], cache_shape, 1.0),
    }


def layer_norm(x, ln_w):
    x_f32 = x.astype(jnp.float32)
    centered = x_f32 - jnp.mean(x_f32, axis=-1, keepdims=True)
    variance = jnp.mean(centered * centered, axis=-1, keepdims=True)
    return (centered * lax.rsqrt(variance + LN_EPS) * ln_w.astype(jnp.float32)).astype(jnp.bfloat16)


def reference(x, seq_len, ln_w, w_q, w_o, w_gate, w_up, w_down, k_cache, v_cache):
    group_size = Q_HEADS // KV_HEADS
    hidden = layer_norm(x, ln_w)
    query = jnp.dot(hidden, w_q, preferred_element_type=jnp.float32).astype(jnp.bfloat16)
    positions = jnp.arange(SEQ_LEN)

    def attend(operands):
        q_rows, k_rows, v_rows, length = operands
        scores = jnp.dot(q_rows.astype(jnp.float32), k_rows.astype(jnp.float32).T) * HEAD_DIM ** -0.5
        scores = jnp.where(positions[None, :] <= length, scores, -jnp.inf)
        probs = jax.nn.softmax(scores, axis=-1)
        return jnp.dot(probs, v_rows.astype(jnp.float32))

    attn_heads = lax.map(attend, (
        query.reshape(BATCH_ROWS * KV_HEADS, group_size, HEAD_DIM),
        k_cache.reshape(BATCH_ROWS * KV_HEADS, SEQ_LEN, HEAD_DIM),
        v_cache.reshape(BATCH_ROWS * KV_HEADS, SEQ_LEN, HEAD_DIM),
        jnp.repeat(seq_len, KV_HEADS)))
    attn_vals = attn_heads.reshape(BATCH_ROWS, Q_HEADS * HEAD_DIM).astype(jnp.bfloat16)
    attn_proj = jnp.dot(attn_vals, w_o, preferred_element_type=jnp.float32)
    gate_proj = jnp.dot(hidden, w_gate, preferred_element_type=jnp.float32)
    up_proj = jnp.dot(hidden, w_up, preferred_element_type=jnp.float32)
    act_vals = (jax.nn.silu(gate_proj) * up_proj).astype(jnp.bfloat16)
    mlp_proj = jnp.dot(act_vals, w_down, preferred_element_type=jnp.float32)
    x_out = (x.astype(jnp.float32) + attn_proj + mlp_proj).astype(jnp.bfloat16)
    return x_out
```

```python
import functools

import jax
import jax.numpy as jnp
from jax import lax
from jax.experimental import pallas as pl
from jax.experimental.pallas import tpu as pltpu
from jax.sharding import PartitionSpec as P

LN_EPS = 1e-5
NEG_BIG = -1e30
MESH = pl.DeviceIdType.MESH
SIDE = 4
N_SP = SIDE ** 3
N_GROUP = 16
LANES = 128
Q_CHUNKS = 8


def coords(sp):
    return lax.div(sp, 16), lax.rem(lax.div(sp, 4), 4), lax.rem(sp, 4)


def octant(z, y, x):
    return 4 * lax.div(z, 2) + 2 * lax.div(y, 2) + lax.div(x, 2)


def corner(z, y, x):
    return 4 * lax.rem(z, 2) + 2 * lax.rem(y, 2) + lax.rem(x, 2)


def far_first(n):
    return n + lax.div(n, 2) * (5 - 2 * n)


def kernel(seq_ref, x_hbm, lnw_hbm, wq_hbm, wo_hbm, wg_hbm, wu_hbm, wd_hbm, k_hbm, v_hbm, out_ref,
           x_v, lnw_v, h_v, wq_v, k_v, v_v, wg_v, wu_v, wd_v, wo_v, q_v, part_v, row_v,
           att_send, att_recv, sum_send, sum_recv, fin,
           x_sem, wq_sem, k_sem, v_sem, wg_sem, wu_sem, wd_sem, wo_sem,
           att_ss, att_rs, sum_ss, sum_rs, fin_ss, fin_rs):
    n_rows, width = x_v.shape
    n_kv, seq_block, head_dim = k_v.shape[1:]
    n_heads = q_v.shape[0] // n_rows
    inner = wg_v.shape[1]
    o_rows = wo_v.shape[0]
    q_rows = wq_v.shape[1]
    piece = width // N_GROUP
    piece_rows = piece // LANES
    tp = lax.axis_index('tp')
    sp = lax.axis_index('sp')
    z, y, x = coords(sp)
    row = octant(z, y, x)
    hp = corner(z, y, x)
    member = hp * 2 + tp

    barrier = pltpu.get_barrier_semaphore()

    def tell(i, c):
        flat = lax.rem(sp * 2 + tp + i, 2 * N_SP)
        pl.semaphore_signal(barrier, inc=1, device_id={'tp': lax.rem(flat, 2), 'sp': lax.div(flat, 2)},
                            device_id_type=MESH)
        return c

    def wq_copy(i):
        return pltpu.make_async_copy(wq_hbm.at[pl.ds(i * q_rows, q_rows)], wq_v.at[i], wq_sem.at[i])

    def k_copy(b):
        return pltpu.make_async_copy(k_hbm.at[b], k_v.at[b], k_sem.at[b])

    def v_copy(b):
        return pltpu.make_async_copy(v_hbm.at[b], v_v.at[b], v_sem.at[b])

    up_rows = width // 8
    inner_at = pl.multiple_of(hp * inner, LANES)

    def wg_copy(i):
        at = pl.ds(i * up_rows, up_rows)
        return pltpu.make_async_copy(wg_hbm.at[at, pl.ds(inner_at, inner)], wg_v.at[at], wg_sem.at[i])

    def wu_copy(i):
        at = pl.ds(i * up_rows, up_rows)
        return pltpu.make_async_copy(wu_hbm.at[at, pl.ds(inner_at, inner)], wu_v.at[at], wu_sem.at[i])

    wd_copy = pltpu.make_async_copy(wd_hbm.at[pl.ds(inner_at, inner)], wd_v, wd_sem)
    wo_copy = pltpu.make_async_copy(wo_hbm.at[pl.ds(pl.multiple_of(hp * o_rows, o_rows), o_rows)], wo_v, wo_sem)

    x_copy = pltpu.make_async_copy(x_hbm, x_v, x_sem.at[0])
    lnw_copy = pltpu.make_async_copy(lnw_hbm, lnw_v, x_sem.at[1])
    x_copy.start()
    lnw_copy.start()
    for i in range(Q_CHUNKS):
        wq_copy(i).start()
    lax.fori_loop(1, 2 * N_SP, tell, 0)

    x_copy.wait()
    lnw_copy.wait()
    x_f32 = x_v[...].astype(jnp.float32)
    centered = x_f32 - jnp.mean(x_f32, axis=-1, keepdims=True)
    variance = jnp.mean(centered * centered, axis=-1, keepdims=True)
    hidden = centered * lax.rsqrt(variance + LN_EPS) * lnw_v[...].astype(jnp.float32)
    h_v[...] = hidden.astype(jnp.bfloat16)

    def q_step(i, acc):
        k_copy(i).start()
        v_copy(i).start()
        wq_copy(i).wait()
        at = pl.multiple_of(i * q_rows, q_rows)
        return acc + jnp.dot(h_v[:, pl.ds(at, q_rows)], wq_v[i], preferred_element_type=jnp.float32)

    query = lax.fori_loop(0, Q_CHUNKS, q_step, jnp.zeros((n_rows, n_heads * head_dim), jnp.float32))
    query = query.astype(jnp.bfloat16).astype(jnp.float32)
    for h in range(n_heads):
        q_v[h * n_rows:(h + 1) * n_rows, :] = query[:, h * head_dim:(h + 1) * head_dim]

    first_kv = lax.broadcasted_iota(jnp.int32, (8, head_dim), 0) < 4
    positions = sp * seq_block + lax.broadcasted_iota(jnp.int32, (8, seq_block), 1)

    def att_step(b, c):
        wg_copy(b).start()
        wu_copy(b).start()
        k_copy(b).wait()
        v_copy(b).wait()
        is_live = positions <= seq_ref[b]
        for j in range(n_kv // 2):
            q8 = q_v[pl.ds(j * 8 * n_rows + b, 8, stride=n_rows), :]
            zero = jnp.zeros_like(q8)
            q_wide = jnp.concatenate([jnp.where(first_kv, q8, zero), jnp.where(first_kv, zero, q8)], axis=1)
            k_wide = jnp.concatenate([k_v[b, 2 * j], k_v[b, 2 * j + 1]], axis=1)
            v_wide = jnp.concatenate([v_v[b, 2 * j], v_v[b, 2 * j + 1]], axis=1)
            scores = lax.dot_general(q_wide.astype(jnp.bfloat16), k_wide, (((1,), (1,)), ((), ())),
                                     preferred_element_type=jnp.float32) * head_dim ** -0.5
            scores = jnp.where(is_live, scores, NEG_BIG)
            block_max = jnp.max(scores, axis=-1, keepdims=True)
            probs = jnp.where(is_live, jnp.exp(scores - block_max), 0.0)
            block_sum = jnp.sum(probs, axis=-1, keepdims=True)
            wide = jnp.dot(probs.astype(jnp.bfloat16), v_wide, preferred_element_type=jnp.float32)
            any_live = block_sum > 0.0
            safe_sum = jnp.where(any_live, block_sum, 1.0)
            o8 = jnp.where(first_kv, wide[:, :head_dim], wide[:, head_dim:]) / safe_sum
            lse = jnp.where(any_live, block_max + jnp.log(safe_sum), NEG_BIG)
            lse8 = jnp.broadcast_to(lse, (8, head_dim))
            for r in range(4):
                att_send[b, j * 4 + r, 0:2, :] = o8[2 * r:2 * r + 2]
                att_send[b, j * 4 + r, 2:4, :] = lse8[2 * r:2 * r + 2]
        return c

    lax.fori_loop(0, n_rows, att_step, 0)
    wd_copy.start()
    wo_copy.start()

    pl.semaphore_wait(barrier, 2 * N_SP - 1)

    def att_exchange(i, c):
        n = N_SP - 1 - i
        dz, dy, dx = coords(n)
        pz = lax.rem(z + far_first(dz), SIDE)
        py = lax.rem(y + far_first(dy), SIDE)
        px = lax.rem(x + far_first(dx), SIDE)
        pltpu.make_async_remote_copy(
            src_ref=att_send.at[octant(pz, py, px), corner(pz, py, px)], dst_ref=att_recv.at[sp],
            send_sem=att_ss, recv_sem=att_rs,
            device_id={'tp': tp, 'sp': pz * 16 + py * 4 + px}, device_id_type=MESH).start()
        return c

    lax.fori_loop(0, N_SP - 1, att_exchange, 0)
    att_recv[sp] = att_send[row, hp]

    def up_step(i, acc):
        wg_copy(i).wait()
        wu_copy(i).wait()
        at = pl.multiple_of(i * up_rows, up_rows)
        h = h_v[:, pl.ds(at, up_rows)]
        return (acc[0] + jnp.dot(h, wg_v[pl.ds(at, up_rows), :], preferred_element_type=jnp.float32),
                acc[1] + jnp.dot(h, wu_v[pl.ds(at, up_rows), :], preferred_element_type=jnp.float32))

    start = jnp.zeros((n_rows, inner), jnp.float32)
    gate, up = lax.fori_loop(0, 8, up_step, (start, start))
    act = (gate * jax.nn.sigmoid(gate) * up).astype(jnp.bfloat16)
    wd_copy.wait()
    down_cols = width // 8

    def down_step(i, c):
        at = pl.ds(pl.multiple_of(i * down_cols, down_cols), down_cols)
        part_v[:, at] = jnp.dot(act, wd_v[:, at], preferred_element_type=jnp.float32)
        return c

    lax.fori_loop(0, 8, down_step, 0)
    wo_copy.wait()

    others = att_recv.at[pl.ds(0, N_SP - 1)]
    pltpu.make_async_copy(others, others, att_rs).wait()
    lse = att_recv[:, 2:4, :]
    weight = jnp.exp(lse - jnp.max(lse, axis=0, keepdims=True))
    attn = jnp.sum(att_recv[:, 0:2, :] * weight, axis=0) / jnp.sum(weight, axis=0)
    attn = jnp.concatenate([attn[0:1], attn[1:2]], axis=1)
    is_row = lax.broadcasted_iota(jnp.int32, (n_rows, 2 * head_dim), 0) == row
    attn = jnp.where(is_row, jnp.broadcast_to(attn, is_row.shape), 0.0).astype(jnp.bfloat16)

    is_mine = lax.broadcasted_iota(jnp.int32, (n_rows, down_cols), 0) == row

    def out_step(i, c):
        at = pl.ds(pl.multiple_of(i * down_cols, down_cols), down_cols)
        total = part_v[:, at] + jnp.dot(attn, wo_v[:, at], preferred_element_type=jnp.float32)
        row_v[:, at] = jnp.sum(jnp.where(is_mine, total, 0.0), axis=0, keepdims=True)
        return c

    lax.fori_loop(0, 8, out_step, 0)

    for m in range(N_GROUP):
        for r in range(piece_rows):
            sum_send[m, r:r + 1, :] = row_v[:, m * piece + r * LANES:m * piece + (r + 1) * LANES]

    def sum_exchange(i, c):
        n = N_GROUP - 1 - i
        ptp = lax.rem(tp + lax.rem(n, 2), 2)
        pz = 2 * lax.div(z, 2) + lax.rem(lax.rem(z, 2) + lax.div(n, 8), 2)
        py = 2 * lax.div(y, 2) + lax.rem(lax.rem(y, 2) + lax.rem(lax.div(n, 4), 2), 2)
        px = 2 * lax.div(x, 2) + lax.rem(lax.rem(x, 2) + lax.rem(lax.div(n, 2), 2), 2)
        pltpu.make_async_remote_copy(
            src_ref=sum_send.at[corner(pz, py, px) * 2 + ptp], dst_ref=sum_recv.at[member],
            send_sem=sum_ss, recv_sem=sum_rs,
            device_id={'tp': ptp, 'sp': pz * 16 + py * 4 + px}, device_id_type=MESH).start()
        return c

    lax.fori_loop(0, N_GROUP - 1, sum_exchange, 0)
    sum_recv[member] = sum_send[member]
    pieces = sum_recv.at[pl.ds(0, N_GROUP - 1)]
    pltpu.make_async_copy(pieces, pieces, sum_rs).wait()
    slot = row * N_GROUP + member
    fin[slot] = jnp.sum(sum_recv[...], axis=0)

    def fin_exchange(i, c):
        n = 2 * N_SP - 1 - i
        dz, dy, dx = coords(lax.div(n, 2))
        pz = lax.rem(z + far_first(dz), SIDE)
        py = lax.rem(y + far_first(dy), SIDE)
        px = lax.rem(x + far_first(dx), SIDE)
        pltpu.make_async_remote_copy(
            src_ref=fin.at[slot], dst_ref=fin.at[slot], send_sem=fin_ss, recv_sem=fin_rs,
            device_id={'tp': lax.rem(tp + lax.rem(n, 2), 2), 'sp': pz * 16 + py * 4 + px}, device_id_type=MESH).start()
        return c

    lax.fori_loop(0, 2 * N_SP - 1, fin_exchange, 0)
    arrived = fin.at[pl.ds(0, 2 * N_SP - 1)]
    pltpu.make_async_copy(arrived, arrived, fin_rs).wait()
    for c in range(width // LANES):
        m, r = c // piece_rows, c % piece_rows
        rows = jnp.concatenate([fin[b * N_GROUP + m, r:r + 1, :] for b in range(n_rows)], axis=0)
        at = slice(c * LANES, (c + 1) * LANES)
        out_ref[:, at] = x_v[:, at].astype(jnp.float32) + rows

    pltpu.make_async_copy(others, others, att_ss).wait()
    pltpu.make_async_copy(pieces, pieces, sum_ss).wait()
    pltpu.make_async_copy(arrived, arrived, fin_ss).wait()


def solution(mesh):
    cache_spec = P(None, 'tp', 'sp', None)
    col_spec = P(None, 'tp')
    row_spec = P('tp', None)

    def local_step(x, seq_len, ln_w, w_q, w_o, w_gate, w_up, w_down, k_cache, v_cache):
        n_rows, n_kv, seq_block, head_dim = k_cache.shape
        width = x.shape[1]
        q_width = w_q.shape[1]
        inner = w_gate.shape[1] // 8
        piece_rows = width // N_GROUP // LANES
        hbm = pl.BlockSpec(memory_space=pl.ANY)
        dma = pltpu.SemaphoreType.DMA
        total = pl.pallas_call(
            kernel,
            out_shape=jax.ShapeDtypeStruct((n_rows, width), jnp.float32),
            in_specs=[pl.BlockSpec(memory_space=pltpu.SMEM)] + [hbm] * 9,
            out_specs=pl.BlockSpec(memory_space=pltpu.VMEM),
            scratch_shapes=[
                pltpu.VMEM((n_rows, width), jnp.bfloat16),
                pltpu.VMEM((1, width), jnp.bfloat16),
                pltpu.VMEM((n_rows, width), jnp.bfloat16),
                pltpu.VMEM((Q_CHUNKS, width // Q_CHUNKS, q_width), jnp.bfloat16),
                pltpu.VMEM(k_cache.shape, jnp.bfloat16),
                pltpu.VMEM(v_cache.shape, jnp.bfloat16),
                pltpu.VMEM((width, inner), jnp.bfloat16),
                pltpu.VMEM((width, inner), jnp.bfloat16),
                pltpu.VMEM((inner, width), jnp.bfloat16),
                pltpu.VMEM((q_width // 8, width), jnp.bfloat16),
                pltpu.VMEM((n_rows * q_width // head_dim, head_dim), jnp.float32),
                pltpu.VMEM((n_rows, width), jnp.float32),
                pltpu.VMEM((1, width), jnp.float32),
                pltpu.VMEM((n_rows, 8, 4, LANES), jnp.float32),
                pltpu.VMEM((N_SP, 4, LANES), jnp.float32),
                pltpu.VMEM((N_GROUP, piece_rows, LANES), jnp.float32),
                pltpu.VMEM((N_GROUP, piece_rows, LANES), jnp.float32),
                pltpu.VMEM((2 * N_SP, piece_rows, LANES), jnp.float32),
                dma((2,)), dma((Q_CHUNKS,)), dma((8,)), dma((8,)), dma((8,)), dma((8,)), dma, dma,
                dma, dma, dma, dma, dma, dma,
            ],
            compiler_params=pltpu.CompilerParams(
                collective_id=0, has_side_effects=True, vmem_limit_bytes=60 * 1024 * 1024),
        )(seq_len, x, ln_w.reshape(1, width), w_q, w_o, w_gate, w_up, w_down, k_cache, v_cache)
        return total.astype(jnp.bfloat16)

    return jax.shard_map(local_step, mesh=mesh,
                         in_specs=(P(), P(), P(), col_spec, row_spec,
                                   col_spec, col_spec, row_spec, cache_spec, cache_spec),
                         out_specs=P(), check_vma=False)
```

```python
import jax
import jax.numpy as jnp
from jax import lax
from jax.experimental import pallas as pl
from jax.experimental.pallas import tpu as pltpu
from jax.sharding import PartitionSpec as P

LN_EPS = 1e-5
NEG_BIG = -1e30
MESH = pl.DeviceIdType.MESH
SIDE = 4
N_SP = SIDE ** 3
N_CHIPS = 8
N_GROUP = 2 * N_CHIPS
LANES = 128
Q_CHUNKS = 8


def hops(d):
    return min(d, SIDE - d)


STEPS = sorted(((dz, dy, dx) for dz in range(SIDE) for dy in range(SIDE) for dx in range(SIDE) if dz or dy or dx),
               key=lambda s: -sum(hops(d) for d in s))
FLIPS = sorted(((fz, fy, fx) for fz in range(2) for fy in range(2) for fx in range(2) if fz or fy or fx),
               key=lambda s: -sum(s))


def kernel(seq_ref, x_hbm, lnw_hbm, wq_hbm, wo_hbm, wg_hbm, wu_hbm, wd_hbm, k_hbm, v_hbm, out_ref,
           x_v, lnw_v, h_v, wq_v, k_v, v_v, wg_v, wu_v, wd_v, wo_v, q_v, s_v, p_v, stat_v, part_v,
           att_send, att_recv, sum_send, sum_recv, fin,
           x_sem, wq_sem, k_sem, v_sem, wg_sem, wu_sem, wd_sem, wo_sem,
           att_ss, att_rs, sum_ss, sum_rs, fin_ss, fin_rs):
    n_rows, width = x_v.shape
    n_kv, seq_block, head_dim = k_v.shape[1:]
    n_heads = q_v.shape[0] // n_rows
    inner = wg_v.shape[1]
    o_rows = wo_v.shape[0]
    q_rows = wq_v.shape[1]
    n_sets = n_rows * n_kv // 2
    piece = width // N_CHIPS
    piece_rows = piece // LANES
    up_rows = width // 8
    tp = lax.axis_index('tp')
    sp = lax.axis_index('sp')
    z, y, x = lax.div(sp, 16), lax.rem(lax.div(sp, 4), 4), lax.rem(sp, 4)
    zs, ys, xs = ([lax.rem(c + d, SIDE) for d in range(SIDE)] for c in (z, y, x))
    to_z = [32 * lax.div(c, 2) + 4 * lax.rem(c, 2) for c in zs]
    to_y = [16 * lax.div(c, 2) + 2 * lax.rem(c, 2) for c in ys]
    to_x = [8 * lax.div(c, 2) + lax.rem(c, 2) for c in xs]
    mine = to_z[0] + to_y[0] + to_x[0]
    row, corner = lax.div(mine, N_CHIPS), lax.rem(mine, N_CHIPS)
    at_z, at_y = [16 * c for c in zs], [4 * c for c in ys]
    flip_z, flip_y, flip_x = ([c, c + 1 - 2 * lax.rem(c, 2)] for c in (z, y, x))

    def step_to(s):
        return at_z[s[0]] + at_y[s[1]] + xs[s[2]]

    def flip_to(f):
        return 16 * flip_z[f[0]] + 4 * flip_y[f[1]] + flip_x[f[2]]

    def wq_copy(i):
        return pltpu.make_async_copy(wq_hbm.at[pl.ds(i * q_rows, q_rows)], wq_v.at[i], wq_sem.at[i])

    def k_copy(b):
        return pltpu.make_async_copy(k_hbm.at[b], k_v.at[b], k_sem.at[b])

    def v_copy(b):
        return pltpu.make_async_copy(v_hbm.at[b], v_v.at[b], v_sem.at[b])

    inner_at = pl.multiple_of(corner * inner, LANES)

    def wg_copy(i):
        at = pl.ds(i * up_rows, up_rows)
        return pltpu.make_async_copy(wg_hbm.at[at, pl.ds(inner_at, inner)], wg_v.at[at], wg_sem.at[i])

    def wu_copy(i):
        at = pl.ds(i * up_rows, up_rows)
        return pltpu.make_async_copy(wu_hbm.at[at, pl.ds(inner_at, inner)], wu_v.at[at], wu_sem.at[i])

    wd_copy = pltpu.make_async_copy(wd_hbm.at[pl.ds(inner_at, inner)], wd_v, wd_sem)
    wo_copy = pltpu.make_async_copy(wo_hbm.at[pl.ds(pl.multiple_of(corner * o_rows, o_rows), o_rows)], wo_v, wo_sem)
    x_copy = pltpu.make_async_copy(x_hbm, x_v, x_sem.at[0])
    lnw_copy = pltpu.make_async_copy(lnw_hbm, lnw_v, x_sem.at[1])

    with jax.named_scope('entry'):
        x_copy.start()
        lnw_copy.start()
        for i in range(Q_CHUNKS):
            wq_copy(i).start()
        barrier = pltpu.get_barrier_semaphore()
        for s in STEPS:
            pl.semaphore_signal(barrier, inc=1, device_id={'tp': tp, 'sp': step_to(s)}, device_id_type=MESH)
        for f in FLIPS + [(0, 0, 0)]:
            pl.semaphore_signal(barrier, inc=1, device_id={'tp': 1 - tp, 'sp': flip_to(f)}, device_id_type=MESH)

    with jax.named_scope('wait_x'):
        x_copy.wait()
    with jax.named_scope('wait_lnw'):
        lnw_copy.wait()
    with jax.named_scope('norm'):
        x_f32 = x_v[...].astype(jnp.float32)
        centered = x_f32 - jnp.mean(x_f32, axis=-1, keepdims=True)
        variance = jnp.mean(centered * centered, axis=-1, keepdims=True)
        scale = lnw_v[...].astype(jnp.float32).reshape(1, width)
        h_v[...] = (centered * lax.rsqrt(variance + LN_EPS) * scale).astype(jnp.bfloat16)

    with jax.named_scope('query'):
        def q_step(i, acc):
            k_copy(i).start()
            v_copy(i).start()
            wq_copy(i).wait()
            at = pl.multiple_of(i * q_rows, q_rows)
            return acc + jnp.dot(h_v[:, pl.ds(at, q_rows)], wq_v[i], preferred_element_type=jnp.float32)

        query = lax.fori_loop(0, Q_CHUNKS, q_step, jnp.zeros((n_rows, n_heads * head_dim), jnp.float32))
        query = query.astype(jnp.bfloat16).astype(jnp.float32)
        for h in range(n_heads):
            q_v[h * n_rows:(h + 1) * n_rows, :] = query[:, h * head_dim:(h + 1) * head_dim]

    first_kv = lax.broadcasted_iota(jnp.int32, (8, head_dim), 0) < 4
    positions = sp * seq_block + lax.broadcasted_iota(jnp.int32, (8, seq_block), 1)

    with jax.named_scope('wait_k'):
        for i in range(8):
            wg_copy(i).start()
            wu_copy(i).start()
        for b in range(n_rows):
            k_copy(b).wait()
    with jax.named_scope('scores'):
        for c in range(n_sets):
            b, j = c // (n_kv // 2), c % (n_kv // 2)
            q8 = q_v[pl.ds(j * 8 * n_rows + b, 8, stride=n_rows), :]
            zero = jnp.zeros_like(q8)
            q_wide = jnp.concatenate([jnp.where(first_kv, q8, zero), jnp.where(first_kv, zero, q8)], axis=1)
            k_wide = jnp.concatenate([k_v[b, 2 * j], k_v[b, 2 * j + 1]], axis=1)
            s_v[8 * c:8 * c + 8, :] = lax.dot_general(q_wide.astype(jnp.bfloat16), k_wide, (((1,), (1,)), ((), ())),
                                                      preferred_element_type=jnp.float32)
    with jax.named_scope('softmax'):
        for c in range(n_sets):
            is_live = positions <= seq_ref[c // (n_kv // 2)]
            scores = jnp.where(is_live, s_v[8 * c:8 * c + 8, :] * head_dim ** -0.5, NEG_BIG)
            block_max = jnp.max(scores, axis=-1, keepdims=True)
            probs = jnp.where(is_live, jnp.exp(scores - block_max), 0.0)
            block_sum = jnp.sum(probs, axis=-1, keepdims=True)
            p_v[8 * c:8 * c + 8, :] = probs
            any_live = block_sum > 0.0
            safe_sum = jnp.where(any_live, block_sum, 1.0)
            lse = jnp.broadcast_to(jnp.where(any_live, block_max + jnp.log(safe_sum), NEG_BIG), (8, head_dim))
            stat_v[8 * c:8 * c + 8, :] = jnp.broadcast_to(1.0 / safe_sum, (8, head_dim))
            b, j = c // (n_kv // 2), c % (n_kv // 2)
            for r in range(4):
                att_send[b * 8 + j * 4 + r, 2:4, :] = lse[2 * r:2 * r + 2]
    with jax.named_scope('wait_v'):
        for b in range(n_rows):
            v_copy(b).wait()
    with jax.named_scope('values'):
        for c in range(n_sets):
            b, j = c // (n_kv // 2), c % (n_kv // 2)
            v_wide = jnp.concatenate([v_v[b, 2 * j], v_v[b, 2 * j + 1]], axis=1)
            wide = jnp.dot(p_v[8 * c:8 * c + 8, :].astype(jnp.bfloat16), v_wide, preferred_element_type=jnp.float32)
            o8 = jnp.where(first_kv, wide[:, :head_dim], wide[:, head_dim:]) * stat_v[8 * c:8 * c + 8, :]
            for r in range(4):
                att_send[b * 8 + j * 4 + r, 0:2, :] = o8[2 * r:2 * r + 2]

    with jax.named_scope('att_send'):
        wd_copy.start()
        wo_copy.start()
        pl.semaphore_wait(barrier, N_SP - 1 + N_CHIPS)
        for s in STEPS:
            pltpu.make_async_remote_copy(
                src_ref=att_send.at[to_z[s[0]] + to_y[s[1]] + to_x[s[2]]], dst_ref=att_recv.at[sp],
                send_sem=att_ss, recv_sem=att_rs,
                device_id={'tp': tp, 'sp': step_to(s)}, device_id_type=MESH).start()
        att_recv[sp] = att_send[mine]

    with jax.named_scope('mlp'):
        def up_step(i, acc):
            wg_copy(i).wait()
            wu_copy(i).wait()
            at = pl.multiple_of(i * up_rows, up_rows)
            h = h_v[:, pl.ds(at, up_rows)]
            return (acc[0] + jnp.dot(h, wg_v[pl.ds(at, up_rows), :], preferred_element_type=jnp.float32),
                    acc[1] + jnp.dot(h, wu_v[pl.ds(at, up_rows), :], preferred_element_type=jnp.float32))

        start = jnp.zeros((n_rows, inner), jnp.float32)
        gate, up = lax.fori_loop(0, 8, up_step, (start, start))
        act = (gate * jax.nn.sigmoid(gate) * up).astype(jnp.bfloat16)
        wd_copy.wait()
        part_cols = width // 4

        def down_step(i, c):
            at = pl.ds(pl.multiple_of(i * part_cols, part_cols), part_cols)
            part_v[:, at] = jnp.dot(act, wd_v[:, at], preferred_element_type=jnp.float32)
            return c

        lax.fori_loop(0, 4, down_step, 0)
        wo_copy.wait()

    others = att_recv.at[pl.ds(0, N_SP - 1)]
    with jax.named_scope('att_wait'):
        pltpu.make_async_copy(others, others, att_rs).wait()
    with jax.named_scope('combine'):
        lse = att_recv[:, 2:4, :]
        weight = jnp.exp(lse - jnp.max(lse, axis=0, keepdims=True))
        attn = jnp.sum(att_recv[:, 0:2, :] * weight, axis=0) / jnp.sum(weight, axis=0)
        attn = jnp.concatenate([attn[0:1], attn[1:2]], axis=1)
        is_row = lax.broadcasted_iota(jnp.int32, (n_rows, 2 * head_dim), 0) == row
        attn = jnp.where(is_row, jnp.broadcast_to(attn, is_row.shape), 0.0).astype(jnp.bfloat16)
        is_mine = lax.broadcasted_iota(jnp.int32, (n_rows, piece), 0) == row
    with jax.named_scope('out_proj'):
        for c in range(N_CHIPS):
            at = slice(c * piece, (c + 1) * piece)
            total = part_v[:, at] + jnp.dot(attn, wo_v[:, at], preferred_element_type=jnp.float32)
            total = jnp.sum(jnp.where(is_mine, total, 0.0), axis=0, keepdims=True)
            for r in range(piece_rows):
                sum_send[c, r:r + 1, :] = total[:, r * LANES:(r + 1) * LANES]

    with jax.named_scope('sum_send'):
        member = corner * 2 + tp
        for f in FLIPS + [(0, 0, 0)]:
            to = flip_to(f)
            piece_of = (4 * lax.rem(flip_z[f[0]], 2) + 2 * lax.rem(flip_y[f[1]], 2) + lax.rem(flip_x[f[2]], 2))
            for ptp in ((tp, 1 - tp) if any(f) else (1 - tp,)):
                pltpu.make_async_remote_copy(
                    src_ref=sum_send.at[piece_of], dst_ref=sum_recv.at[member], send_sem=sum_ss, recv_sem=sum_rs,
                    device_id={'tp': ptp, 'sp': to}, device_id_type=MESH).start()
        sum_recv[member] = sum_send[corner]
    pieces = sum_recv.at[pl.ds(0, N_GROUP - 1)]
    with jax.named_scope('sum_wait'):
        pltpu.make_async_copy(pieces, pieces, sum_rs).wait()

    with jax.named_scope('fin_send'):
        fin[mine] = jnp.sum(sum_recv[...], axis=0)
        for s in STEPS:
            pltpu.make_async_remote_copy(
                src_ref=fin.at[mine], dst_ref=fin.at[mine], send_sem=fin_ss, recv_sem=fin_rs,
                device_id={'tp': tp, 'sp': step_to(s)}, device_id_type=MESH).start()
    arrived = fin.at[pl.ds(0, N_SP - 1)]
    with jax.named_scope('fin_wait'):
        pltpu.make_async_copy(arrived, arrived, fin_rs).wait()
    with jax.named_scope('finish'):
        for c in range(width // LANES):
            m, r = c // piece_rows, c % piece_rows
            rows = jnp.concatenate([fin[b * N_CHIPS + m, r:r + 1, :] for b in range(n_rows)], axis=0)
            at = slice(c * LANES, (c + 1) * LANES)
            out_ref[:, at] = (x_v[:, at].astype(jnp.float32) + rows).astype(jnp.bfloat16)
    with jax.named_scope('drain'):
        pltpu.make_async_copy(others, others, att_ss).wait()
        pltpu.make_async_copy(pieces, pieces, sum_ss).wait()
        pltpu.make_async_copy(arrived, arrived, fin_ss).wait()


def solution(mesh):
    cache_spec = P(None, 'tp', 'sp', None)
    col_spec = P(None, 'tp')
    row_spec = P('tp', None)

    def local_step(x, seq_len, ln_w, w_q, w_o, w_gate, w_up, w_down, k_cache, v_cache):
        n_rows, n_kv, seq_block, head_dim = k_cache.shape
        width = x.shape[1]
        q_width = w_q.shape[1]
        inner = w_gate.shape[1] // N_CHIPS
        piece_rows = width // N_CHIPS // LANES
        n_queries = n_rows * q_width // head_dim
        hbm = pl.BlockSpec(memory_space=pl.ANY)
        dma = pltpu.SemaphoreType.DMA
        return pl.pallas_call(
            kernel,
            out_shape=jax.ShapeDtypeStruct((n_rows, width), jnp.bfloat16),
            in_specs=[pl.BlockSpec(memory_space=pltpu.SMEM)] + [hbm] * 9,
            out_specs=pl.BlockSpec(memory_space=pltpu.VMEM),
            scratch_shapes=[
                pltpu.VMEM((n_rows, width), jnp.bfloat16),
                pltpu.VMEM((width,), jnp.bfloat16),
                pltpu.VMEM((n_rows, width), jnp.bfloat16),
                pltpu.VMEM((Q_CHUNKS, width // Q_CHUNKS, q_width), jnp.bfloat16),
                pltpu.VMEM(k_cache.shape, jnp.bfloat16),
                pltpu.VMEM(v_cache.shape, jnp.bfloat16),
                pltpu.VMEM((width, inner), jnp.bfloat16),
                pltpu.VMEM((width, inner), jnp.bfloat16),
                pltpu.VMEM((inner, width), jnp.bfloat16),
                pltpu.VMEM((q_width // N_CHIPS, width), jnp.bfloat16),
                pltpu.VMEM((n_queries, head_dim), jnp.float32),
                pltpu.VMEM((n_queries, seq_block), jnp.float32),
                pltpu.VMEM((n_queries, seq_block), jnp.float32),
                pltpu.VMEM((n_queries, head_dim), jnp.float32),
                pltpu.VMEM((n_rows, width), jnp.float32),
                pltpu.VMEM((N_SP, 4, LANES), jnp.float32),
                pltpu.VMEM((N_SP, 4, LANES), jnp.float32),
                pltpu.VMEM((N_CHIPS, piece_rows, LANES), jnp.float32),
                pltpu.VMEM((N_GROUP, piece_rows, LANES), jnp.float32),
                pltpu.VMEM((N_SP, piece_rows, LANES), jnp.float32),
                dma((2,)), dma((Q_CHUNKS,)), dma((8,)), dma((8,)), dma((8,)), dma((8,)), dma, dma,
                dma, dma, dma, dma, dma, dma,
            ],
            compiler_params=pltpu.CompilerParams(
                collective_id=0, has_side_effects=True, vmem_limit_bytes=60 * 1024 * 1024),
        )(seq_len, x, ln_w, w_q, w_o, w_gate, w_up, w_down, k_cache, v_cache)

    return jax.shard_map(local_step, mesh=mesh,
                         in_specs=(P(), P(), P(), col_spec, row_spec,
                                   col_spec, col_spec, row_spec, cache_spec, cache_spec),
                         out_specs=P(), check_vma=False)
```

```python
import jax
import jax.numpy as jnp
from jax import lax
from jax.experimental import pallas as pl
from jax.experimental.pallas import tpu as pltpu
from jax.sharding import PartitionSpec as P

LN_EPS = 1e-5
NEG_BIG = -1e30
MESH = pl.DeviceIdType.MESH
SIDE = 4
N_SP = SIDE ** 3
N_CHIPS = 8
N_GROUP = 2 * N_CHIPS
LANES = 128
Q_CHUNKS = 8
N_INNER = 48


def hops(d):
    return min(d, SIDE - d)


STEPS = sorted(((dz, dy, dx) for dz in range(SIDE) for dy in range(SIDE) for dx in range(SIDE) if dz or dy or dx),
               key=lambda s: -sum(hops(d) for d in s))
FLIPS = sorted(((fz, fy, fx) for fz in range(2) for fy in range(2) for fx in range(2) if fz or fy or fx),
               key=lambda s: -sum(s))


def kernel(seq_hbm, x_hbm, lnw_hbm, wq_hbm, wo_hbm, wg_hbm, wu_hbm, wd_hbm, k_hbm, v_hbm, out_ref,
           seq_ref, x_v, lnw_v, h_v, wq_v, k_v, v_v, wg_v, wu_v, wd_v, wo_v, q_v, s_v, p_v, stat_v,
           att_send, att_recv, mlp_send, mlp_recv, half_send, half_recv, sum_send, sum_recv, fin,
           x_sem, wq_sem, k_sem, v_sem, wg_sem, wu_sem, wd_sem, wo_sem,
           att_ss, att_rs, mlp_ss, mlp_rs, half_ss, half_rs, sum_ss, sum_rs, fin_ss, fin_rs):
    n_rows, width = x_v.shape
    n_kv, seq_block, head_dim = k_v.shape[1:]
    n_heads = q_v.shape[0] // n_rows
    inner = wg_v.shape[1]
    o_rows = wo_v.shape[0]
    q_rows = width // Q_CHUNKS
    n_sets = n_rows * n_kv // 2
    piece = width // N_CHIPS
    piece_rows = piece // LANES
    tp = lax.axis_index('tp')
    sp = lax.axis_index('sp')
    z, y, x = lax.div(sp, 16), lax.rem(lax.div(sp, 4), 4), lax.rem(sp, 4)
    zs, ys, xs = ([lax.rem(c + d, SIDE) for d in range(SIDE)] for c in (z, y, x))
    to_z = [32 * lax.div(c, 2) + 4 * lax.rem(c, 2) for c in zs]
    to_y = [16 * lax.div(c, 2) + 2 * lax.rem(c, 2) for c in ys]
    to_x = [8 * lax.div(c, 2) + lax.rem(c, 2) for c in xs]
    mine = to_z[0] + to_y[0] + to_x[0]
    row, corner = lax.div(mine, N_CHIPS), lax.rem(mine, N_CHIPS)
    at_z, at_y = [16 * c for c in zs], [4 * c for c in ys]
    flip_z, flip_y, flip_x = ([c, c + 1 - 2 * lax.rem(c, 2)] for c in (z, y, x))

    def step_to(s):
        return at_z[s[0]] + at_y[s[1]] + xs[s[2]]

    def flip_to(f):
        return 16 * flip_z[f[0]] + 4 * flip_y[f[1]] + flip_x[f[2]]

    def wq_copy(i):
        at = pl.ds(i * q_rows, q_rows)
        return pltpu.make_async_copy(wq_hbm.at[at], wq_v.at[at], wq_sem.at[i])

    half_rows = q_rows // 2

    def wq_half(i):
        at = pl.ds(width - (2 - i) * half_rows, half_rows)
        return pltpu.make_async_copy(wq_hbm.at[at], wq_v.at[at], wq_sem.at[Q_CHUNKS - 1 + i])

    def k_copy(b):
        return pltpu.make_async_copy(k_hbm.at[b], k_v.at[b], k_sem.at[b])

    def v_copy(b):
        return pltpu.make_async_copy(v_hbm.at[b], v_v.at[b], v_sem.at[b])

    inner_at = pl.multiple_of(lax.rem(sp, N_INNER) * inner, LANES)
    wg_copy = pltpu.make_async_copy(wg_hbm.at[:, pl.ds(inner_at, inner)], wg_v, wg_sem)
    wu_copy = pltpu.make_async_copy(wu_hbm.at[:, pl.ds(inner_at, inner)], wu_v, wu_sem)
    wd_copy = pltpu.make_async_copy(wd_hbm.at[pl.ds(inner_at, inner)], wd_v, wd_sem)
    wo_copy = pltpu.make_async_copy(wo_hbm.at[pl.ds(pl.multiple_of(corner * o_rows, o_rows), o_rows)], wo_v, wo_sem)
    x_copy = pltpu.make_async_copy(x_hbm, x_v, x_sem.at[0])
    lnw_copy = pltpu.make_async_copy(lnw_hbm, lnw_v, x_sem.at[1])
    seq_copy = pltpu.make_async_copy(seq_hbm, seq_ref, x_sem.at[2])

    with jax.named_scope('entry'):
        barrier = pltpu.get_barrier_semaphore()

        def tell(to_tp, to_sp):
            pl.semaphore_signal(barrier, inc=1, device_id={'tp': to_tp, 'sp': to_sp}, device_id_type=MESH)

        x_copy.start()
        lnw_copy.start()
        tell(1 - tp, sp)
        for i in range(Q_CHUNKS - 1):
            wq_copy(i).start()
        wq_half(0).start()
        wq_half(1).start()
        seq_copy.start()
        for s in STEPS[:32]:
            tell(tp, step_to(s))
        for b in range(n_rows):
            k_copy(b).start()
        for s in STEPS[32:]:
            tell(tp, step_to(s))
        for b in range(n_rows):
            v_copy(b).start()
        for f in FLIPS:
            tell(1 - tp, flip_to(f))
        wg_copy.start()
        wu_copy.start()

    with jax.named_scope('wait_x'):
        x_copy.wait()
    with jax.named_scope('wait_lnw'):
        lnw_copy.wait()
    with jax.named_scope('norm'):
        x_f32 = x_v[...].astype(jnp.float32)
        centered = x_f32 - jnp.mean(x_f32, axis=-1, keepdims=True)
        variance = jnp.mean(centered * centered, axis=-1, keepdims=True)
        scale = lnw_v[...].astype(jnp.float32).reshape(1, width)
        h_v[...] = (centered * lax.rsqrt(variance + LN_EPS) * scale).astype(jnp.bfloat16)

    with jax.named_scope('query'):
        def q_step(i, acc):
            wq_copy(i).wait()
            at = pl.ds(pl.multiple_of(i * q_rows, q_rows), q_rows)
            return acc + jnp.dot(h_v[:, at], wq_v[at, :], preferred_element_type=jnp.float32)

        query = lax.fori_loop(0, Q_CHUNKS - 1, q_step, jnp.zeros((n_rows, n_heads * head_dim), jnp.float32))
        for i in range(2):
            wq_half(i).wait()
            at = slice(width - (2 - i) * half_rows, width - (1 - i) * half_rows)
            query += jnp.dot(h_v[:, at], wq_v[at, :], preferred_element_type=jnp.float32)
        query = query.astype(jnp.bfloat16).astype(jnp.float32)
        for h in range(n_heads):
            q_v[h * n_rows:(h + 1) * n_rows, :] = query[:, h * head_dim:(h + 1) * head_dim]

    first_kv = lax.broadcasted_iota(jnp.int32, (8, head_dim), 0) < 4
    positions = sp * seq_block + lax.broadcasted_iota(jnp.int32, (8, seq_block), 1)

    with jax.named_scope('scores'):
        wd_copy.start()
        wo_copy.start()
        seq_copy.wait()
        for c in range(n_sets):
            b, j = c // (n_kv // 2), c % (n_kv // 2)
            if c % (n_sets // 2) == 0:
                for i in range(n_rows // 2):
                    k_copy(b + i).wait()
            q8 = q_v[pl.ds(j * 8 * n_rows + b, 8, stride=n_rows), :]
            zero = jnp.zeros_like(q8)
            q_wide = jnp.concatenate([jnp.where(first_kv, q8, zero), jnp.where(first_kv, zero, q8)], axis=1)
            k_wide = jnp.concatenate([k_v[b, 2 * j], k_v[b, 2 * j + 1]], axis=1)
            s_v[8 * c:8 * c + 8, :] = lax.dot_general(q_wide.astype(jnp.bfloat16), k_wide, (((1,), (1,)), ((), ())),
                                                      preferred_element_type=jnp.float32)
    with jax.named_scope('softmax'):
        for c in range(n_sets):
            is_live = positions <= seq_ref[c // (n_kv // 2)]
            scores = jnp.where(is_live, s_v[8 * c:8 * c + 8, :] * head_dim ** -0.5, NEG_BIG)
            block_max = jnp.max(scores, axis=-1, keepdims=True)
            probs = jnp.where(is_live, jnp.exp(scores - block_max), 0.0)
            block_sum = jnp.sum(probs, axis=-1, keepdims=True)
            p_v[8 * c:8 * c + 8, :] = probs
            any_live = block_sum > 0.0
            safe_sum = jnp.where(any_live, block_sum, 1.0)
            lse = jnp.broadcast_to(jnp.where(any_live, block_max + jnp.log(safe_sum), NEG_BIG), (8, head_dim))
            stat_v[8 * c:8 * c + 8, :] = jnp.broadcast_to(1.0 / safe_sum, (8, head_dim))
            b, j = c // (n_kv // 2), c % (n_kv // 2)
            for r in range(4):
                att_send[b * 8 + j * 4 + r, 2:4, :] = lse[2 * r:2 * r + 2]
    with jax.named_scope('values'):
        for c in range(n_sets):
            b, j = c // (n_kv // 2), c % (n_kv // 2)
            if c % (n_sets // 2) == 0:
                for i in range(n_rows // 2):
                    v_copy(b + i).wait()
            v_wide = jnp.concatenate([v_v[b, 2 * j], v_v[b, 2 * j + 1]], axis=1)
            wide = jnp.dot(p_v[8 * c:8 * c + 8, :].astype(jnp.bfloat16), v_wide, preferred_element_type=jnp.float32)
            o8 = jnp.where(first_kv, wide[:, :head_dim], wide[:, head_dim:]) * stat_v[8 * c:8 * c + 8, :]
            for r in range(4):
                att_send[b * 8 + j * 4 + r, 0:2, :] = o8[2 * r:2 * r + 2]

    with jax.named_scope('att_send'):
        pl.semaphore_wait(barrier, N_SP - 1 + N_CHIPS)
        for s in STEPS:
            pltpu.make_async_remote_copy(
                src_ref=att_send.at[to_z[s[0]] + to_y[s[1]] + to_x[s[2]]], dst_ref=att_recv.at[sp],
                send_sem=att_ss, recv_sem=att_rs,
                device_id={'tp': tp, 'sp': step_to(s)}, device_id_type=MESH).start()
        att_recv[sp] = att_send[mine]

    with jax.named_scope('mlp'):
        wg_copy.wait()
        wu_copy.wait()
        wd_copy.wait()

        @pl.when(sp < N_INNER)
        def _():
            up_wide = jnp.concatenate([wg_v[...], wu_v[...]], axis=1)
            wide = jnp.dot(h_v[...], up_wide, preferred_element_type=jnp.float32)
            gate, up = wide[:, :inner], wide[:, inner:]
            act = (gate * jax.nn.sigmoid(gate) * up).astype(jnp.bfloat16)
            for c in range(N_CHIPS):
                part = jnp.dot(act, wd_v[:, c * piece:(c + 1) * piece], preferred_element_type=jnp.float32)
                for b in range(n_rows):
                    for r in range(piece_rows):
                        mlp_send[b * N_CHIPS + c, r:r + 1, :] = part[b:b + 1, r * LANES:(r + 1) * LANES]

    with jax.named_scope('mlp_send'):
        @pl.when(sp < N_INNER)
        def _():
            for s in STEPS:
                pltpu.make_async_remote_copy(
                    src_ref=mlp_send.at[to_z[s[0]] + to_y[s[1]] + to_x[s[2]]], dst_ref=mlp_recv.at[sp],
                    send_sem=mlp_ss, recv_sem=mlp_rs,
                    device_id={'tp': tp, 'sp': step_to(s)}, device_id_type=MESH).start()
            mlp_recv[sp] = mlp_send[mine]

        wo_copy.wait()

    others = att_recv.at[pl.ds(0, N_SP - 1)]
    with jax.named_scope('att_wait'):
        pltpu.make_async_copy(others, others, att_rs).wait()
    with jax.named_scope('combine'):
        lse = att_recv[:, 2:4, :]
        weight = jnp.exp(lse - jnp.max(lse, axis=0, keepdims=True))
        attn = jnp.sum(att_recv[:, 0:2, :] * weight, axis=0) / jnp.sum(weight, axis=0)
        attn = jnp.concatenate([attn[0:1], attn[1:2]], axis=1)
        is_row = lax.broadcasted_iota(jnp.int32, (n_rows, 2 * head_dim), 0) == row
        attn = jnp.where(is_row, jnp.broadcast_to(attn, is_row.shape), 0.0).astype(jnp.bfloat16)
        is_mine = lax.broadcasted_iota(jnp.int32, (n_rows, piece), 0) == row
    with jax.named_scope('out_proj'):
        for c in range(N_CHIPS):
            at = slice(c * piece, (c + 1) * piece)
            total = jnp.dot(attn, wo_v[:, at], preferred_element_type=jnp.float32)
            total = jnp.sum(jnp.where(is_mine, total, 0.0), axis=0, keepdims=True)
            for r in range(piece_rows):
                sum_send[c, r:r + 1, :] = total[:, r * LANES:(r + 1) * LANES]

    with jax.named_scope('sum_send'):
        member = corner * 2 + tp
        for f in FLIPS + [(0, 0, 0)]:
            to = flip_to(f)
            piece_of = (4 * lax.rem(flip_z[f[0]], 2) + 2 * lax.rem(flip_y[f[1]], 2) + lax.rem(flip_x[f[2]], 2))
            for ptp in ((tp, 1 - tp) if any(f) else (1 - tp,)):
                pltpu.make_async_remote_copy(
                    src_ref=sum_send.at[piece_of], dst_ref=sum_recv.at[member], send_sem=sum_ss, recv_sem=sum_rs,
                    device_id={'tp': ptp, 'sp': to}, device_id_type=MESH).start()
        sum_recv[member] = sum_send[corner]
    with jax.named_scope('mlp_wait'):
        for is_sender in (True, False):
            @pl.when((sp < N_INNER) == is_sender)
            def _():
                heard = mlp_recv.at[pl.ds(0, N_INNER - is_sender)]
                pltpu.make_async_copy(heard, heard, mlp_rs).wait()

    with jax.named_scope('half_send'):
        half_send[...] = jnp.sum(mlp_recv[...], axis=0)
        half_copy = pltpu.make_async_remote_copy(
            src_ref=half_send, dst_ref=half_recv, send_sem=half_ss, recv_sem=half_rs,
            device_id={'tp': 1 - tp, 'sp': sp}, device_id_type=MESH)
        half_copy.start()
    pieces = sum_recv.at[pl.ds(0, N_GROUP - 1)]
    with jax.named_scope('sum_wait'):
        pltpu.make_async_copy(pieces, pieces, sum_rs).wait()
    with jax.named_scope('half_wait'):
        half_copy.wait_recv()

    with jax.named_scope('fin_send'):
        fin[mine] = jnp.sum(sum_recv[...], axis=0) + (half_send[...] + half_recv[...])
        for s in STEPS:
            pltpu.make_async_remote_copy(
                src_ref=fin.at[mine], dst_ref=fin.at[mine], send_sem=fin_ss, recv_sem=fin_rs,
                device_id={'tp': tp, 'sp': step_to(s)}, device_id_type=MESH).start()
    arrived = fin.at[pl.ds(0, N_SP - 1)]
    with jax.named_scope('fin_wait'):
        pltpu.make_async_copy(arrived, arrived, fin_rs).wait()
    with jax.named_scope('finish'):
        for c in range(width // LANES):
            m, r = c // piece_rows, c % piece_rows
            rows = jnp.concatenate([fin[b * N_CHIPS + m, r:r + 1, :] for b in range(n_rows)], axis=0)
            at = slice(c * LANES, (c + 1) * LANES)
            out_ref[:, at] = (x_v[:, at].astype(jnp.float32) + rows).astype(jnp.bfloat16)
    with jax.named_scope('drain'):
        pltpu.make_async_copy(others, others, att_ss).wait()
        half_copy.wait_send()

        @pl.when(sp < N_INNER)
        def _():
            sent = mlp_send.at[pl.ds(0, N_SP - 1)]
            pltpu.make_async_copy(sent, sent, mlp_ss).wait()

        pltpu.make_async_copy(pieces, pieces, sum_ss).wait()
        pltpu.make_async_copy(arrived, arrived, fin_ss).wait()


def solution(mesh):
    cache_spec = P(None, 'tp', 'sp', None)
    col_spec = P(None, 'tp')
    row_spec = P('tp', None)

    def local_step(x, seq_len, ln_w, w_q, w_o, w_gate, w_up, w_down, k_cache, v_cache):
        n_rows, n_kv, seq_block, head_dim = k_cache.shape
        width = x.shape[1]
        q_width = w_q.shape[1]
        inner = w_gate.shape[1] // N_INNER
        piece_rows = width // N_CHIPS // LANES
        n_queries = n_rows * q_width // head_dim
        hbm = pl.BlockSpec(memory_space=pltpu.HBM)
        dma = pltpu.SemaphoreType.DMA
        return pl.pallas_call(
            kernel,
            out_shape=jax.ShapeDtypeStruct((n_rows, width), jnp.bfloat16),
            in_specs=[hbm] * 10,
            out_specs=pl.BlockSpec(memory_space=pltpu.VMEM),
            scratch_shapes=[
                pltpu.SMEM((n_rows,), jnp.int32),
                pltpu.VMEM((n_rows, width), jnp.bfloat16),
                pltpu.VMEM((width,), jnp.bfloat16),
                pltpu.VMEM((n_rows, width), jnp.bfloat16),
                pltpu.VMEM((width, q_width), jnp.bfloat16),
                pltpu.VMEM(k_cache.shape, jnp.bfloat16),
                pltpu.VMEM(v_cache.shape, jnp.bfloat16),
                pltpu.VMEM((width, inner), jnp.bfloat16),
                pltpu.VMEM((width, inner), jnp.bfloat16),
                pltpu.VMEM((inner, width), jnp.bfloat16),
                pltpu.VMEM((q_width // N_CHIPS, width), jnp.bfloat16),
                pltpu.VMEM((n_queries, head_dim), jnp.float32),
                pltpu.VMEM((n_queries, seq_block), jnp.float32),
                pltpu.VMEM((n_queries, seq_block), jnp.float32),
                pltpu.VMEM((n_queries, head_dim), jnp.float32),
                pltpu.VMEM((N_SP, 4, LANES), jnp.float32),
                pltpu.VMEM((N_SP, 4, LANES), jnp.float32),
                pltpu.VMEM((N_SP, piece_rows, LANES), jnp.float32),
                pltpu.VMEM((N_INNER, piece_rows, LANES), jnp.float32),
                pltpu.VMEM((piece_rows, LANES), jnp.float32),
                pltpu.VMEM((piece_rows, LANES), jnp.float32),
                pltpu.VMEM((N_CHIPS, piece_rows, LANES), jnp.float32),
                pltpu.VMEM((N_GROUP, piece_rows, LANES), jnp.float32),
                pltpu.VMEM((N_SP, piece_rows, LANES), jnp.float32),
                dma((3,)), dma((Q_CHUNKS + 1,)), dma((8,)), dma((8,)), dma, dma, dma, dma,
                dma, dma, dma, dma,
                dma, dma, dma, dma, dma, dma,
            ],
            compiler_params=pltpu.CompilerParams(
                collective_id=0, has_side_effects=True, vmem_limit_bytes=40 * 1024 * 1024),
        )(*(pltpu.with_memory_space_constraint(a, pltpu.HBM)
            for a in (seq_len, x, ln_w, w_q, w_o, w_gate, w_up, w_down, k_cache, v_cache)))

    return jax.shard_map(local_step, mesh=mesh,
                         in_specs=(P(), P(), P(), col_spec, row_spec,
                                   col_spec, col_spec, row_spec, cache_spec, cache_spec),
                         out_specs=P(), check_vma=False)
```

```python
import jax
import jax.numpy as jnp
from jax import lax
from jax.experimental import pallas as pl
from jax.experimental.pallas import tpu as pltpu
from jax.sharding import PartitionSpec as P

LN_EPS = 1e-5
NEG_BIG = -1e30
MESH = pl.DeviceIdType.MESH
SIDE = 4
N_SP = SIDE ** 3
N_CHIPS = 8
N_GROUP = 2 * N_CHIPS
LANES = 128
Q_CHUNKS = 8
N_INNER = 48


def hops(d):
    return min(d, SIDE - d)


STEPS = sorted(((dz, dy, dx) for dz in range(SIDE) for dy in range(SIDE) for dx in range(SIDE) if dz or dy or dx),
               key=lambda s: -sum(hops(d) for d in s))
COMBINE_ORDER = (
    0, 16, 4, 1, 3, 12, 20, 32, 2, 8, 17, 19, 5, 28, 7, 24,
    36, 18, 21, 33, 48, 6, 9, 13, 15, 23, 35, 40, 44, 11, 29, 34,
    10, 14, 31, 37, 52, 22, 25, 27, 39, 49, 51, 56, 26, 30, 38, 41,
    43, 45, 47, 50, 60, 42, 46, 53, 55, 54, 57, 59, 61, 63, 58, 62,
)
FINISH_ORDER = (
    0, 3, 12, 4, 1, 16, 2, 8, 15, 48, 7, 32, 19, 11, 13, 28,
    14, 5, 20, 51, 17, 6, 35, 60, 9, 44, 18, 24, 31, 10, 52, 49,
    23, 36, 50, 33, 56, 63, 34, 29, 40, 47, 27, 21, 30, 55, 22, 39,
    61, 25, 59, 45, 53, 62, 26, 43, 46, 37, 54, 38, 57, 41, 58, 42,
)
FLIPS = sorted(((fz, fy, fx) for fz in range(2) for fy in range(2) for fx in range(2) if fz or fy or fx),
               key=lambda s: -sum(s))


def slot_of(sp):
    z, y, x = sp // 16, sp // 4 % 4, sp % 4
    return 32 * (z // 2) + 4 * (z % 2) + 16 * (y // 2) + 2 * (y % 2) + 8 * (x // 2) + x % 2


def kernel(seq_hbm, x_hbm, lnw_hbm, wq_hbm, wo_hbm, wg_hbm, wu_hbm, wd_hbm, k_hbm, v_hbm, out_ref,
           seq_ref, x_v, lnw_v, h_v, wq_v, k_v, v_v, wg_v, wu_v, wd_v, wo_v, q_v, s_v, p_v, stat_v,
           att_send, att_recv, mlp_send, mlp_recv, half_send, half_recv, sum_send, sum_recv, fin,
           x_sem, wq_sem, k_sem, v_sem, wg_sem, wu_sem, wd_sem, wo_sem,
           att_ss, att_rs, mlp_ss, mlp_rs, half_ss, half_rs, sum_ss, sum_rs, fin_ss, fin_rs):
    n_rows, width = x_v.shape
    n_kv, seq_block, head_dim = k_v.shape[1:]
    n_heads = q_v.shape[0] // n_rows
    inner = wg_v.shape[1]
    o_rows = wo_v.shape[0]
    q_rows = width // Q_CHUNKS
    n_sets = n_rows * n_kv // 2
    piece = width // N_CHIPS
    piece_rows = piece // LANES
    tp = lax.axis_index('tp')
    sp = lax.axis_index('sp')
    z, y, x = lax.div(sp, 16), lax.rem(lax.div(sp, 4), 4), lax.rem(sp, 4)
    zs, ys, xs = ([lax.rem(c + d, SIDE) for d in range(SIDE)] for c in (z, y, x))
    mine = (32 * lax.div(z, 2) + 4 * lax.rem(z, 2) + 16 * lax.div(y, 2) + 2 * lax.rem(y, 2)
            + 8 * lax.div(x, 2) + lax.rem(x, 2))
    row, corner = lax.div(mine, N_CHIPS), lax.rem(mine, N_CHIPS)
    at_z, at_y = [16 * c for c in zs], [4 * c for c in ys]
    flip_z, flip_y, flip_x = ([c, c + 1 - 2 * lax.rem(c, 2)] for c in (z, y, x))

    def step_to(s):
        return at_z[s[0]] + at_y[s[1]] + xs[s[2]]

    def in_order(order):
        for to in order[:-1]:
            is_me = sp == to
            yield jnp.where(is_me, order[-1], to), jnp.where(is_me, slot_of(order[-1]), slot_of(to))

    def flip_to(f):
        return 16 * flip_z[f[0]] + 4 * flip_y[f[1]] + flip_x[f[2]]

    def wq_copy(i):
        at = pl.ds(i * q_rows, q_rows)
        return pltpu.make_async_copy(wq_hbm.at[at], wq_v.at[at], wq_sem.at[i])

    half_rows = q_rows // 2

    def wq_half(i):
        at = pl.ds(width - (2 - i) * half_rows, half_rows)
        return pltpu.make_async_copy(wq_hbm.at[at], wq_v.at[at], wq_sem.at[Q_CHUNKS - 1 + i])

    def k_copy(b):
        return pltpu.make_async_copy(k_hbm.at[b], k_v.at[b], k_sem.at[b])

    def v_copy(b):
        return pltpu.make_async_copy(v_hbm.at[b], v_v.at[b], v_sem.at[b])

    inner_at = pl.multiple_of(lax.rem(sp, N_INNER) * inner, LANES)
    wg_copy = pltpu.make_async_copy(wg_hbm.at[:, pl.ds(inner_at, inner)], wg_v, wg_sem)
    wu_copy = pltpu.make_async_copy(wu_hbm.at[:, pl.ds(inner_at, inner)], wu_v, wu_sem)
    wd_copy = pltpu.make_async_copy(wd_hbm.at[pl.ds(inner_at, inner)], wd_v, wd_sem)
    wo_copy = pltpu.make_async_copy(wo_hbm.at[pl.ds(pl.multiple_of(corner * o_rows, o_rows), o_rows)], wo_v, wo_sem)
    x_copy = pltpu.make_async_copy(x_hbm, x_v, x_sem.at[0])
    lnw_copy = pltpu.make_async_copy(lnw_hbm, lnw_v, x_sem.at[1])
    seq_copy = pltpu.make_async_copy(seq_hbm, seq_ref, x_sem.at[2])

    with jax.named_scope('entry'):
        barrier = pltpu.get_barrier_semaphore()

        def tell(to_tp, to_sp):
            pl.semaphore_signal(barrier, inc=1, device_id={'tp': to_tp, 'sp': to_sp}, device_id_type=MESH)

        x_copy.start()
        lnw_copy.start()
        tell(1 - tp, sp)
        for i in range(Q_CHUNKS - 1):
            wq_copy(i).start()
        wq_half(0).start()
        wq_half(1).start()
        seq_copy.start()
        for s in STEPS[:32]:
            tell(tp, step_to(s))
        for b in range(n_rows):
            k_copy(b).start()
        for s in STEPS[32:]:
            tell(tp, step_to(s))
        for b in range(n_rows):
            v_copy(b).start()
        for f in FLIPS:
            tell(1 - tp, flip_to(f))
        wg_copy.start()
        wu_copy.start()

    with jax.named_scope('wait_x'):
        x_copy.wait()
    with jax.named_scope('wait_lnw'):
        lnw_copy.wait()
    with jax.named_scope('norm'):
        x_f32 = x_v[...].astype(jnp.float32)
        centered = x_f32 - jnp.mean(x_f32, axis=-1, keepdims=True)
        variance = jnp.mean(centered * centered, axis=-1, keepdims=True)
        scale = lnw_v[...].astype(jnp.float32).reshape(1, width)
        h_v[...] = (centered * lax.rsqrt(variance + LN_EPS) * scale).astype(jnp.bfloat16)

    with jax.named_scope('query'):
        def q_step(i, acc):
            wq_copy(i).wait()
            at = pl.ds(pl.multiple_of(i * q_rows, q_rows), q_rows)
            return acc + jnp.dot(h_v[:, at], wq_v[at, :], preferred_element_type=jnp.float32)

        query = lax.fori_loop(0, Q_CHUNKS - 1, q_step, jnp.zeros((n_rows, n_heads * head_dim), jnp.float32))
        for i in range(2):
            wq_half(i).wait()
            at = slice(width - (2 - i) * half_rows, width - (1 - i) * half_rows)
            query += jnp.dot(h_v[:, at], wq_v[at, :], preferred_element_type=jnp.float32)
        query = query.astype(jnp.bfloat16).astype(jnp.float32)
        for h in range(n_heads):
            q_v[h * n_rows:(h + 1) * n_rows, :] = query[:, h * head_dim:(h + 1) * head_dim]

    first_kv = lax.broadcasted_iota(jnp.int32, (8, head_dim), 0) < 4
    positions = sp * seq_block + lax.broadcasted_iota(jnp.int32, (8, seq_block), 1)

    low_lanes = lax.broadcasted_iota(jnp.int32, (1, head_dim), 1) < head_dim // 2
    per_row = n_kv // 2
    with jax.named_scope('scores'):
        wd_copy.start()
        wo_copy.start()
        seq_copy.wait()
        for g in range(0, n_rows, 2):
            k_copy(g).wait()
            k_copy(g + 1).wait()
            sets = range(g * per_row, (g + 2) * per_row)
            for c in sets:
                b, j = c // per_row, c % per_row
                q8 = q_v[pl.ds(j * 8 * n_rows + b, 8, stride=n_rows), :]
                zero = jnp.zeros_like(q8)
                q_wide = jnp.concatenate([jnp.where(first_kv, q8, zero), jnp.where(first_kv, zero, q8)], axis=1)
                k_wide = jnp.concatenate([k_v[b, 2 * j], k_v[b, 2 * j + 1]], axis=1)
                s_v[8 * c:8 * c + 8, :] = lax.dot_general(q_wide.astype(jnp.bfloat16), k_wide, (((1,), (1,)), ((), ())),
                                                          preferred_element_type=jnp.float32)
            for c in sets:
                b, j = c // per_row, c % per_row
                is_live = positions <= seq_ref[b]
                scores = jnp.where(is_live, s_v[8 * c:8 * c + 8, :] * head_dim ** -0.5, NEG_BIG)
                block_max = jnp.max(scores, axis=-1, keepdims=True)
                probs = jnp.where(is_live, jnp.exp(scores - block_max), 0.0)
                block_sum = jnp.sum(probs, axis=-1, keepdims=True)
                p_v[8 * c:8 * c + 8, :] = probs
                any_live = block_sum > 0.0
                safe_sum = jnp.where(any_live, block_sum, 1.0)
                lse = jnp.broadcast_to(jnp.where(any_live, block_max + jnp.log(safe_sum), NEG_BIG), (8, head_dim))
                stat_v[8 * c:8 * c + 8, :] = jnp.broadcast_to(1.0 / safe_sum, (8, head_dim))
                for r in range(4):
                    att_send[b * 8 + j * 4 + r, 2:3, :] = jnp.where(low_lanes, lse[2 * r:2 * r + 1], lse[2 * r + 1:2 * r + 2])
    with jax.named_scope('values'):
        for g, n in ((0, 2), (2, 2), (4, 2), (6, 1), (7, 1)):
            for b in range(g, g + n):
                v_copy(b).wait()
            for c in range(g * per_row, (g + n) * per_row):
                b, j = c // per_row, c % per_row
                v_wide = jnp.concatenate([v_v[b, 2 * j], v_v[b, 2 * j + 1]], axis=1)
                wide = jnp.dot(p_v[8 * c:8 * c + 8, :].astype(jnp.bfloat16), v_wide, preferred_element_type=jnp.float32)
                o8 = jnp.where(first_kv, wide[:, :head_dim], wide[:, head_dim:]) * stat_v[8 * c:8 * c + 8, :]
                for r in range(4):
                    att_send[b * 8 + j * 4 + r, 0:2, :] = o8[2 * r:2 * r + 2]

    with jax.named_scope('att_send'):
        pl.semaphore_wait(barrier, N_SP - 1 + N_CHIPS)
        for to, slot in in_order(COMBINE_ORDER):
            pltpu.make_async_remote_copy(
                src_ref=att_send.at[slot, pl.ds(0, 3)], dst_ref=att_recv.at[sp, pl.ds(0, 3)],
                send_sem=att_ss, recv_sem=att_rs,
                device_id={'tp': tp, 'sp': to}, device_id_type=MESH).start()
        att_recv[sp] = att_send[mine]

    with jax.named_scope('mlp'):
        wg_copy.wait()
        wu_copy.wait()
        wd_copy.wait()

        @pl.when(sp < N_INNER)
        def _():
            up_wide = jnp.concatenate([wg_v[...], wu_v[...]], axis=1)
            wide = jnp.dot(h_v[...], up_wide, preferred_element_type=jnp.float32)
            gate, up = wide[:, :inner], wide[:, inner:]
            act = (gate * jax.nn.sigmoid(gate) * up).astype(jnp.bfloat16)
            for c in range(N_CHIPS):
                part = jnp.dot(act, wd_v[:, c * piece:(c + 1) * piece], preferred_element_type=jnp.float32)
                for b in range(n_rows):
                    for r in range(piece_rows):
                        mlp_send[b * N_CHIPS + c, r:r + 1, :] = part[b:b + 1, r * LANES:(r + 1) * LANES]

    with jax.named_scope('mlp_send'):
        @pl.when(sp < N_INNER)
        def _():
            for to, slot in in_order(COMBINE_ORDER):
                pltpu.make_async_remote_copy(
                    src_ref=mlp_send.at[slot], dst_ref=mlp_recv.at[sp], send_sem=mlp_ss, recv_sem=mlp_rs,
                    device_id={'tp': tp, 'sp': to}, device_id_type=MESH).start()
            mlp_recv[sp] = mlp_send[mine]

        wo_copy.wait()

    others = att_recv.at[pl.ds(0, N_SP - 1), pl.ds(0, 3)]
    with jax.named_scope('att_wait'):
        pltpu.make_async_copy(others, others, att_rs).wait()
    with jax.named_scope('combine'):
        lse = att_recv[:, 2, :]
        weight = jnp.exp(lse - jnp.max(lse, axis=0, keepdims=True))
        swapped = pltpu.roll(weight, head_dim // 2, 1)
        attn = []
        for h in range(2):
            spread = jnp.where(low_lanes, weight, swapped) if h == 0 else jnp.where(low_lanes, swapped, weight)
            attn.append(jnp.sum(att_recv[:, h, :] * spread, axis=0, keepdims=True)
                        / jnp.sum(spread, axis=0, keepdims=True))
        attn = jnp.concatenate(attn, axis=1)
        is_row = lax.broadcasted_iota(jnp.int32, (n_rows, 2 * head_dim), 0) == row
        attn = jnp.where(is_row, jnp.broadcast_to(attn, is_row.shape), 0.0).astype(jnp.bfloat16)
        is_mine = lax.broadcasted_iota(jnp.int32, (n_rows, piece), 0) == row
    with jax.named_scope('out_proj'):
        member = corner * 2 + tp
        for f in FLIPS + [(0, 0, 0)]:
            c = 4 * lax.rem(flip_z[f[0]], 2) + 2 * lax.rem(flip_y[f[1]], 2) + lax.rem(flip_x[f[2]], 2)
            at = pl.ds(pl.multiple_of(c * piece, piece), piece)
            total = jnp.dot(attn, wo_v[:, at], preferred_element_type=jnp.float32)
            total = jnp.sum(jnp.where(is_mine, total, 0.0), axis=0, keepdims=True)
            for r in range(piece_rows):
                sum_send[c, r:r + 1, :] = total[:, r * LANES:(r + 1) * LANES]
            for ptp in ((tp, 1 - tp) if any(f) else (1 - tp,)):
                pltpu.make_async_remote_copy(
                    src_ref=sum_send.at[c], dst_ref=sum_recv.at[member], send_sem=sum_ss, recv_sem=sum_rs,
                    device_id={'tp': ptp, 'sp': flip_to(f)}, device_id_type=MESH).start()
        sum_recv[member] = sum_send[corner]

    with jax.named_scope('mlp_wait'):
        for is_sender in (True, False):
            @pl.when((sp < N_INNER) == is_sender)
            def _():
                heard = mlp_recv.at[pl.ds(0, N_INNER - is_sender)]
                pltpu.make_async_copy(heard, heard, mlp_rs).wait()

    with jax.named_scope('half_send'):
        half_send[...] = jnp.sum(mlp_recv[...], axis=0)
        half_copy = pltpu.make_async_remote_copy(
            src_ref=half_send, dst_ref=half_recv, send_sem=half_ss, recv_sem=half_rs,
            device_id={'tp': 1 - tp, 'sp': sp}, device_id_type=MESH)
        half_copy.start()
    pieces = sum_recv.at[pl.ds(0, N_GROUP - 1)]
    with jax.named_scope('sum_wait'):
        pltpu.make_async_copy(pieces, pieces, sum_rs).wait()
    with jax.named_scope('half_wait'):
        half_copy.wait_recv()

    with jax.named_scope('fin_send'):
        fin[mine] = jnp.sum(sum_recv[...], axis=0) + (half_send[...] + half_recv[...])
        for to, _ in in_order(FINISH_ORDER):
            pltpu.make_async_remote_copy(
                src_ref=fin.at[mine], dst_ref=fin.at[mine], send_sem=fin_ss, recv_sem=fin_rs,
                device_id={'tp': tp, 'sp': to}, device_id_type=MESH).start()
    arrived = fin.at[pl.ds(0, N_SP - 1)]
    with jax.named_scope('fin_wait'):
        pltpu.make_async_copy(arrived, arrived, fin_rs).wait()
    with jax.named_scope('finish'):
        for c in range(width // LANES):
            m, r = c // piece_rows, c % piece_rows
            rows = jnp.concatenate([fin[b * N_CHIPS + m, r:r + 1, :] for b in range(n_rows)], axis=0)
            at = slice(c * LANES, (c + 1) * LANES)
            out_ref[:, at] = (x_v[:, at].astype(jnp.float32) + rows).astype(jnp.bfloat16)
    with jax.named_scope('drain'):
        pltpu.make_async_copy(others, others, att_ss).wait()
        half_copy.wait_send()

        @pl.when(sp < N_INNER)
        def _():
            sent = mlp_send.at[pl.ds(0, N_SP - 1)]
            pltpu.make_async_copy(sent, sent, mlp_ss).wait()

        pltpu.make_async_copy(pieces, pieces, sum_ss).wait()
        pltpu.make_async_copy(arrived, arrived, fin_ss).wait()


def solution(mesh):
    cache_spec = P(None, 'tp', 'sp', None)
    col_spec = P(None, 'tp')
    row_spec = P('tp', None)

    def local_step(x, seq_len, ln_w, w_q, w_o, w_gate, w_up, w_down, k_cache, v_cache):
        n_rows, n_kv, seq_block, head_dim = k_cache.shape
        width = x.shape[1]
        q_width = w_q.shape[1]
        inner = w_gate.shape[1] // N_INNER
        piece_rows = width // N_CHIPS // LANES
        n_queries = n_rows * q_width // head_dim
        hbm = pl.BlockSpec(memory_space=pltpu.HBM)
        dma = pltpu.SemaphoreType.DMA
        return pl.pallas_call(
            kernel,
            out_shape=jax.ShapeDtypeStruct((n_rows, width), jnp.bfloat16),
            in_specs=[hbm] * 10,
            out_specs=pl.BlockSpec(memory_space=pltpu.VMEM),
            scratch_shapes=[
                pltpu.SMEM((n_rows,), jnp.int32),
                pltpu.VMEM((n_rows, width), jnp.bfloat16),
                pltpu.VMEM((width,), jnp.bfloat16),
                pltpu.VMEM((n_rows, width), jnp.bfloat16),
                pltpu.VMEM((width, q_width), jnp.bfloat16),
                pltpu.VMEM(k_cache.shape, jnp.bfloat16),
                pltpu.VMEM(v_cache.shape, jnp.bfloat16),
                pltpu.VMEM((width, inner), jnp.bfloat16),
                pltpu.VMEM((width, inner), jnp.bfloat16),
                pltpu.VMEM((inner, width), jnp.bfloat16),
                pltpu.VMEM((q_width // N_CHIPS, width), jnp.bfloat16),
                pltpu.VMEM((n_queries, head_dim), jnp.float32),
                pltpu.VMEM((n_queries, seq_block), jnp.float32),
                pltpu.VMEM((n_queries, seq_block), jnp.float32),
                pltpu.VMEM((n_queries, head_dim), jnp.float32),
                pltpu.VMEM((N_SP, 4, LANES), jnp.float32),
                pltpu.VMEM((N_SP, 4, LANES), jnp.float32),
                pltpu.VMEM((N_SP, piece_rows, LANES), jnp.float32),
                pltpu.VMEM((N_INNER, piece_rows, LANES), jnp.float32),
                pltpu.VMEM((piece_rows, LANES), jnp.float32),
                pltpu.VMEM((piece_rows, LANES), jnp.float32),
                pltpu.VMEM((N_CHIPS, piece_rows, LANES), jnp.float32),
                pltpu.VMEM((N_GROUP, piece_rows, LANES), jnp.float32),
                pltpu.VMEM((N_SP, piece_rows, LANES), jnp.float32),
                dma((3,)), dma((Q_CHUNKS + 1,)), dma((8,)), dma((8,)), dma, dma, dma, dma,
                dma, dma, dma, dma,
                dma, dma, dma, dma, dma, dma,
            ],
            compiler_params=pltpu.CompilerParams(
                collective_id=0, has_side_effects=True, vmem_limit_bytes=40 * 1024 * 1024),
        )(*(pltpu.with_memory_space_constraint(a, pltpu.HBM)
            for a in (seq_len, x, ln_w, w_q, w_o, w_gate, w_up, w_down, k_cache, v_cache)))

    return jax.shard_map(local_step, mesh=mesh,
                         in_specs=(P(), P(), P(), col_spec, row_spec,
                                   col_spec, col_spec, row_spec, cache_spec, cache_spec),
                         out_specs=P(), check_vma=False)
```

```python
import jax
import jax.numpy as jnp
from jax import lax
from jax.experimental import pallas as pl
from jax.experimental.pallas import tpu as pltpu
from jax.sharding import PartitionSpec as P

LN_EPS = 1e-5
NEG_BIG = -1e30
MESH = pl.DeviceIdType.MESH
SIDE = 4
N_SP = SIDE ** 3
N_ROWS = 8
N_PER_ROW = 4
N_COMBINE = N_ROWS * N_PER_ROW
N_GROUP = 2 * N_PER_ROW
N_INNER = 48
LANES = 128
TILE = (8, LANES)
Q_CHUNKS = (1024, 1024, 1024, 512, 256, 256)
V_GROUPS = (4, 3, 1)

FINISH_ORDER = (
    0, 3, 12, 4, 1, 16, 2, 8, 15, 48, 7, 32, 19, 11, 13, 28,
    14, 5, 20, 51, 17, 6, 35, 60, 9, 44, 18, 24, 31, 10, 52, 49,
    23, 36, 50, 33, 56, 63, 34, 29, 40, 47, 27, 21, 30, 55, 22, 39,
    61, 25, 59, 45, 53, 62, 26, 43, 46, 37, 54, 38, 57, 41, 58, 42,
)
ROW_ORDER = (0, 1, 2, 4, 3, 5, 6, 7)


def place(row, part):
    bits = (row // 4, row // 2 % 2, row % 2)
    z, y, x = (3 * b if part == i + 1 else 1 + b for i, b in enumerate(bits))
    return 16 * z + 4 * y + x


STEPS = [(dz, dy, dx) for dz in range(SIDE) for dy in range(SIDE) for dx in range(SIDE) if dz or dy or dx]
FLIPS = [(fz, fy, fx) for fz in range(2) for fy in range(2) for fx in range(2) if fz or fy or fx]


def kernel(seq_hbm, x_hbm, lnw_hbm, wq_hbm, wo_hbm, wg_hbm, wu_hbm, wd_hbm, k_hbm, v_hbm, out_ref,
           seq_ref, x_v, lnw_v, h_v, wq_v, k_v, v_v, wg_v, wu_v, wd_v, wo_v, q_v, s_v, p_v, stat_v, lse_v,
           att_send, att_recv, mlp_send, mlp_recv, half_send, half_recv, sum_send, sum_recv, fin,
           x_sem, wq_sem, k_sem, v_sem, w_sem, send_sem, att_rs, mlp_rs, half_rs, sum_rs, fin_rs):
    n_rows, width = x_v.shape
    n_kv, seq_block, head_dim = k_v.shape[1:]
    n_heads = q_v.shape[0] // n_rows
    inner = wg_v.shape[1]
    o_rows = wo_v.shape[0]
    per_row = n_kv // 2
    piece = width // N_PER_ROW
    tp = lax.axis_index('tp')
    sp = lax.axis_index('sp')
    z, y, x = lax.div(sp, 16), lax.rem(lax.div(sp, 4), 4), lax.rem(sp, 4)
    half_z, half_y, half_x = (lax.div(c, 2) for c in (z, y, x))
    edge_z, edge_y, edge_x = (1 - lax.rem(lax.div(c + 1, 2), 2) for c in (z, y, x))
    combines = edge_z + edge_y + edge_x <= 1
    part = lax.rem(edge_z + 2 * edge_y + 3 * edge_x, N_PER_ROW)
    row = 4 * half_z + 2 * half_y + half_x
    mine = row * N_PER_ROW + part
    shares_mlp = sp < N_INNER

    zs, ys, xs = ([lax.rem(c + d, SIDE) for d in range(SIDE)] for c in (z, y, x))
    at_z, at_y = [16 * c for c in zs], [4 * c for c in ys]
    flip_z, flip_y, flip_x = ([c, c + 1 - 2 * lax.rem(c, 2)] for c in (z, y, x))

    def send(src, dst, kind, sem, to_tp, to_sp):
        pltpu.make_async_remote_copy(src_ref=src, dst_ref=dst, send_sem=send_sem.at[kind], recv_sem=sem,
                                     device_id={'tp': to_tp, 'sp': to_sp}, device_id_type=MESH).start()

    def wait_for(n, sem):
        tiles = att_recv.at[pl.ds(0, n)]
        pltpu.make_async_copy(tiles, tiles, sem).wait()

    def spread(src, dst, sem):
        for r in ROW_ORDER:
            for p in range(N_PER_ROW):
                to = place(r, p)

                @pl.when(sp != to)
                def _():
                    send(src.at[r * N_PER_ROW + p], dst.at[sp], 0, sem, tp, to)

        @pl.when(combines)
        def _():
            dst[sp] = src[mine]

    q_starts = [sum(Q_CHUNKS[:i]) for i in range(len(Q_CHUNKS))]
    v_starts = [sum(V_GROUPS[:i]) for i in range(len(V_GROUPS))]

    def wq_copy(i):
        at = pl.ds(q_starts[i], Q_CHUNKS[i])
        return pltpu.make_async_copy(wq_hbm.at[at], wq_v.at[at], wq_sem.at[i])

    def k_copy(i):
        at = pl.ds(i * (n_rows // 2), n_rows // 2)
        return pltpu.make_async_copy(k_hbm.at[at], k_v.at[at], k_sem.at[i])

    def v_copy(i):
        at = pl.ds(v_starts[i], V_GROUPS[i])
        return pltpu.make_async_copy(v_hbm.at[at], v_v.at[at], v_sem.at[i])

    inner_at = pl.multiple_of(lax.rem(sp, N_INNER) * inner, LANES)
    wg_copy = pltpu.make_async_copy(wg_hbm.at[:, pl.ds(inner_at, inner)], wg_v, w_sem.at[0])
    wu_copy = pltpu.make_async_copy(wu_hbm.at[:, pl.ds(inner_at, inner)], wu_v, w_sem.at[1])
    wd_copy = pltpu.make_async_copy(wd_hbm.at[pl.ds(inner_at, inner)], wd_v, w_sem.at[2])
    wo_copy = pltpu.make_async_copy(wo_hbm.at[pl.ds(pl.multiple_of(part * o_rows, o_rows), o_rows)], wo_v, w_sem.at[3])
    x_copy = pltpu.make_async_copy(x_hbm, x_v, x_sem.at[0])
    lnw_copy = pltpu.make_async_copy(lnw_hbm, lnw_v, x_sem.at[1])
    seq_copy = pltpu.make_async_copy(seq_hbm, seq_ref, x_sem.at[2])

    with jax.named_scope('entry'):
        barrier = pltpu.get_barrier_semaphore()

        def tell(to_tp, to_sp):
            pl.semaphore_signal(barrier, inc=1, device_id={'tp': to_tp, 'sp': to_sp}, device_id_type=MESH)

        x_copy.start()
        lnw_copy.start()
        tell(1 - tp, sp)
        for i in range(len(Q_CHUNKS)):
            wq_copy(i).start()
        seq_copy.start()
        for s in STEPS[:32]:
            tell(tp, at_z[s[0]] + at_y[s[1]] + xs[s[2]])
        k_copy(0).start()
        k_copy(1).start()
        for s in STEPS[32:]:
            tell(tp, at_z[s[0]] + at_y[s[1]] + xs[s[2]])
        for i in range(len(V_GROUPS)):
            v_copy(i).start()
        for f in FLIPS:
            tell(1 - tp, 16 * flip_z[f[0]] + 4 * flip_y[f[1]] + flip_x[f[2]])
        wg_copy.start()
        wu_copy.start()

    with jax.named_scope('wait_x'):
        x_copy.wait()
        lnw_copy.wait()
    with jax.named_scope('norm'):
        x_f32 = x_v[...].astype(jnp.float32)
        centered = x_f32 - jnp.mean(x_f32, axis=-1, keepdims=True)
        variance = jnp.mean(centered * centered, axis=-1, keepdims=True)
        scale = lnw_v[...].astype(jnp.float32).reshape(1, width)
        h_v[...] = (centered * lax.rsqrt(variance + LN_EPS) * scale).astype(jnp.bfloat16)

    with jax.named_scope('query'):
        query = jnp.zeros((n_rows, n_heads * head_dim), jnp.float32)
        for i in range(len(Q_CHUNKS)):
            wq_copy(i).wait()
            at = slice(q_starts[i], q_starts[i] + Q_CHUNKS[i])
            query += jnp.dot(h_v[:, at], wq_v[at, :], preferred_element_type=jnp.float32)
        query = query.astype(jnp.bfloat16).astype(jnp.float32)
        for h in range(n_heads):
            q_v[h * n_rows:(h + 1) * n_rows, :] = query[:, h * head_dim:(h + 1) * head_dim]

    first_kv = lax.broadcasted_iota(jnp.int32, TILE, 0) < 4
    positions = sp * seq_block + lax.broadcasted_iota(jnp.int32, (8, seq_block), 1)

    def score(b, j):
        at = pl.ds((b * per_row + j) * 8, 8)
        q8 = q_v[pl.ds(j * 8 * n_rows + b, 8, stride=n_rows), :]
        zero = jnp.zeros_like(q8)
        q_wide = jnp.concatenate([jnp.where(first_kv, q8, zero), jnp.where(first_kv, zero, q8)], axis=1)
        k_wide = jnp.concatenate([k_v[b, 2 * j], k_v[b, 2 * j + 1]], axis=1)
        s_v[at, :] = lax.dot_general(q_wide.astype(jnp.bfloat16), k_wide, (((1,), (1,)), ((), ())),
                                     preferred_element_type=jnp.float32)

    def soften(b, j):
        at = pl.ds((b * per_row + j) * 8, 8)
        is_live = positions <= seq_ref[b]
        scores = jnp.where(is_live, s_v[at, :] * head_dim ** -0.5, NEG_BIG)
        block_max = jnp.max(scores, axis=-1, keepdims=True)
        probs = jnp.where(is_live, jnp.exp(scores - block_max), 0.0)
        block_sum = jnp.sum(probs, axis=-1, keepdims=True)
        p_v[at, :] = probs
        any_live = block_sum > 0.0
        safe_sum = jnp.where(any_live, block_sum, 1.0)
        lse_v[at, :] = jnp.broadcast_to(jnp.where(any_live, block_max + jnp.log(safe_sum), NEG_BIG), TILE)
        stat_v[at, :] = jnp.broadcast_to(1.0 / safe_sum, TILE)

    def value(b, j):
        at = pl.ds((b * per_row + j) * 8, 8)
        v_wide = jnp.concatenate([v_v[b, 2 * j], v_v[b, 2 * j + 1]], axis=1)
        wide = jnp.dot(p_v[at, :].astype(jnp.bfloat16), v_wide, preferred_element_type=jnp.float32)
        o8 = jnp.where(first_kv, wide[:, :head_dim], wide[:, head_dim:]) * stat_v[at, :]
        lse8 = lse_v[at, :]
        att_send[b * N_PER_ROW + 2 * j] = jnp.where(first_kv, o8, pltpu.roll(lse8, 4, 0))
        att_send[b * N_PER_ROW + 2 * j + 1] = jnp.where(first_kv, pltpu.roll(o8, 4, 0), lse8)

    def sets(start, n):
        return [(b, j) for b in range(start, start + n) for j in range(per_row)]

    with jax.named_scope('scores'):
        wd_copy.start()
        wo_copy.start()
        seq_copy.wait()
        k_copy(0).wait()
        for c in sets(0, n_rows // 2):
            score(*c)
        k_copy(1).wait()
        for c in sets(n_rows // 2, n_rows // 2):
            score(*c)
        for c in sets(0, n_rows // 2):
            soften(*c)
    with jax.named_scope('values'):
        for i in range(len(V_GROUPS)):
            v_copy(i).wait()
            if i == 0:
                for c in sets(n_rows // 2, n_rows // 2):
                    soften(*c)
            for c in sets(v_starts[i], V_GROUPS[i]):
                value(*c)

    with jax.named_scope('att_send'):
        pl.semaphore_wait(barrier, N_SP - 1 + 8)
        spread(att_send, att_recv, att_rs)

    with jax.named_scope('mlp'):
        wg_copy.wait()
        wu_copy.wait()
        wd_copy.wait()

        @pl.when(shares_mlp)
        def _():
            up_wide = jnp.concatenate([wg_v[...], wu_v[...]], axis=1)
            wide = jnp.dot(h_v[...], up_wide, preferred_element_type=jnp.float32)
            gate, up = wide[:, :inner], wide[:, inner:]
            act = (gate * jax.nn.sigmoid(gate) * up).astype(jnp.bfloat16)
            for p in range(N_PER_ROW):
                down = jnp.dot(act, wd_v[:, p * piece:(p + 1) * piece], preferred_element_type=jnp.float32)
                for b in range(n_rows):
                    for r in range(8):
                        mlp_send[b * N_PER_ROW + p, r:r + 1, :] = down[b:b + 1, r * LANES:(r + 1) * LANES]

    with jax.named_scope('mlp_send'):
        @pl.when(shares_mlp)
        def _():
            spread(mlp_send, mlp_recv, mlp_rs)

        wo_copy.wait()

    @pl.when(combines)
    def _():
        with jax.named_scope('att_wait'):
            wait_for(N_SP - 1, att_rs)
        with jax.named_scope('combine'):
            lse = att_recv[:, 4:8, :]
            weight = jnp.exp(lse - jnp.max(lse, axis=0, keepdims=True))
            attn = jnp.sum(att_recv[:, 0:4, :] * weight, axis=0) / jnp.sum(weight, axis=0)
            attn = jnp.concatenate([attn[h:h + 1] for h in range(4)], axis=1)
            is_row = lax.broadcasted_iota(jnp.int32, (n_rows, 4 * head_dim), 0) == row
            attn = jnp.where(is_row, jnp.broadcast_to(attn, is_row.shape), 0.0).astype(jnp.bfloat16)
            is_mine = lax.broadcasted_iota(jnp.int32, (n_rows, piece), 0) == row
        with jax.named_scope('out_proj'):
            for p in range(N_PER_ROW):
                total = jnp.dot(attn, wo_v[:, p * piece:(p + 1) * piece], preferred_element_type=jnp.float32)
                total = jnp.sum(jnp.where(is_mine, total, 0.0), axis=0, keepdims=True)
                for r in range(8):
                    sum_send[p, r:r + 1, :] = total[:, r * LANES:(r + 1) * LANES]

        with jax.named_scope('sum_send'):
            member = part * 2 + tp
            for i in (1, 2, 3, 0):
                p = lax.rem(part + i, N_PER_ROW)
                to = (16 * jnp.where(p == 1, 3 * half_z, 1 + half_z) + 4 * jnp.where(p == 2, 3 * half_y, 1 + half_y)
                      + jnp.where(p == 3, 3 * half_x, 1 + half_x))
                for to_tp in ((tp, 1 - tp) if i else (1 - tp,)):
                    send(sum_send.at[p], sum_recv.at[member], 1, sum_rs, to_tp, to)
            sum_recv[member] = sum_send[part]

        with jax.named_scope('mlp_wait'):
            for is_sender in (True, False):
                @pl.when(shares_mlp == is_sender)
                def _():
                    wait_for(N_INNER - is_sender, mlp_rs)

        with jax.named_scope('half_send'):
            half_send[...] = jnp.sum(mlp_recv[...], axis=0)
            send(half_send, half_recv, 1, half_rs, 1 - tp, sp)
        with jax.named_scope('sum_wait'):
            wait_for(N_GROUP - 1, sum_rs)
        with jax.named_scope('half_wait'):
            wait_for(1, half_rs)

        with jax.named_scope('fin_send'):
            fin[mine] = jnp.sum(sum_recv[...], axis=0) + (half_send[...] + half_recv[...])
            for to in FINISH_ORDER[:-1]:
                send(fin.at[mine], fin.at[mine], 2, fin_rs, tp, jnp.where(sp == to, FINISH_ORDER[-1], to))

    with jax.named_scope('fin_wait'):
        for is_combiner in (True, False):
            @pl.when(combines == is_combiner)
            def _():
                wait_for(N_COMBINE - is_combiner, fin_rs)

    with jax.named_scope('finish'):
        for c in range(width // LANES):
            p, r = c // 8, c % 8
            rows = jnp.concatenate([fin[b * N_PER_ROW + p, r:r + 1, :] for b in range(n_rows)], axis=0)
            at = slice(c * LANES, (c + 1) * LANES)
            out_ref[:, at] = (x_v[:, at].astype(jnp.float32) + rows).astype(jnp.bfloat16)
    with jax.named_scope('drain'):
        for is_combiner in (True, False):
            for is_sender in (True, False):
                @pl.when((combines == is_combiner) & (shares_mlp == is_sender))
                def _():
                    wait_for((N_COMBINE - is_combiner) * (1 + is_sender), send_sem.at[0])

        @pl.when(combines)
        def _():
            wait_for(N_GROUP, send_sem.at[1])
            wait_for(N_SP - 1, send_sem.at[2])


def solution(mesh):
    cache_spec = P(None, 'tp', 'sp', None)
    col_spec = P(None, 'tp')
    row_spec = P('tp', None)

    def local_step(x, seq_len, ln_w, w_q, w_o, w_gate, w_up, w_down, k_cache, v_cache):
        n_rows, n_kv, seq_block, head_dim = k_cache.shape
        width = x.shape[1]
        q_width = w_q.shape[1]
        inner = w_gate.shape[1] // N_INNER
        n_queries = n_rows * q_width // head_dim
        hbm = pl.BlockSpec(memory_space=pltpu.HBM)
        dma = pltpu.SemaphoreType.DMA
        f32, bf16 = jnp.float32, jnp.bfloat16
        return pl.pallas_call(
            kernel,
            out_shape=jax.ShapeDtypeStruct((n_rows, width), bf16),
            in_specs=[hbm] * 10,
            out_specs=pl.BlockSpec(memory_space=pltpu.VMEM),
            scratch_shapes=[
                pltpu.SMEM((n_rows,), jnp.int32),
                pltpu.VMEM((n_rows, width), bf16),
                pltpu.VMEM((width,), bf16),
                pltpu.VMEM((n_rows, width), bf16),
                pltpu.VMEM((width, q_width), bf16),
                pltpu.VMEM(k_cache.shape, bf16),
                pltpu.VMEM(v_cache.shape, bf16),
                pltpu.VMEM((width, inner), bf16),
                pltpu.VMEM((width, inner), bf16),
                pltpu.VMEM((inner, width), bf16),
                pltpu.VMEM((q_width // N_PER_ROW, width), bf16),
                pltpu.VMEM((n_queries, head_dim), f32),
                pltpu.VMEM((n_queries, seq_block), f32),
                pltpu.VMEM((n_queries, seq_block), f32),
                pltpu.VMEM((n_queries, head_dim), f32),
                pltpu.VMEM((n_queries, head_dim), f32),
                pltpu.VMEM((N_COMBINE,) + TILE, f32),
                pltpu.VMEM((N_SP,) + TILE, f32),
                pltpu.VMEM((N_COMBINE,) + TILE, f32),
                pltpu.VMEM((N_INNER,) + TILE, f32),
                pltpu.VMEM(TILE, f32),
                pltpu.VMEM(TILE, f32),
                pltpu.VMEM((N_PER_ROW,) + TILE, f32),
                pltpu.VMEM((N_GROUP,) + TILE, f32),
                pltpu.VMEM((N_COMBINE,) + TILE, f32),
                dma((3,)), dma((len(Q_CHUNKS),)), dma((2,)), dma((len(V_GROUPS),)), dma((4,)),
                dma((3,)), dma, dma, dma, dma, dma,
            ],
            compiler_params=pltpu.CompilerParams(
                collective_id=0, has_side_effects=True, vmem_limit_bytes=44 * 1024 * 1024),
        )(*(pltpu.with_memory_space_constraint(a, pltpu.HBM)
            for a in (seq_len, x, ln_w, w_q, w_o, w_gate, w_up, w_down, k_cache, v_cache)))

    return jax.shard_map(local_step, mesh=mesh,
                         in_specs=(P(), P(), P(), col_spec, row_spec,
                                   col_spec, col_spec, row_spec, cache_spec, cache_spec),
                         out_specs=P(), check_vma=False)
```

```python
import jax
import jax.numpy as jnp
from jax import lax
from jax.experimental import pallas as pl
from jax.experimental.pallas import tpu as pltpu
from jax.sharding import PartitionSpec as P

LN_EPS = 1e-5
NEG_BIG = -1e30
MESH = pl.DeviceIdType.MESH
SIDE = 4
N_SP = SIDE ** 3
N_CHIPS = 8
N_GROUP = 2 * N_CHIPS
LANES = 128
Q_CHUNKS = (1024, 1024, 1024, 512, 256, 256)
V_GROUPS = (4, 3, 1)
N_INNER = 48


def hops(d):
    return min(d, SIDE - d)


STEPS = sorted(((dz, dy, dx) for dz in range(SIDE) for dy in range(SIDE) for dx in range(SIDE) if dz or dy or dx),
               key=lambda s: -sum(hops(d) for d in s))
FINISH_ORDER = (
    0, 3, 12, 4, 1, 16, 2, 8, 15, 48, 7, 32, 19, 11, 13, 28,
    14, 5, 20, 51, 17, 6, 35, 60, 9, 44, 18, 24, 31, 10, 52, 49,
    23, 36, 50, 33, 56, 63, 34, 29, 40, 47, 27, 21, 30, 55, 22, 39,
    61, 25, 59, 45, 53, 62, 26, 43, 46, 37, 54, 38, 57, 41, 58, 42,
)
FLIPS = sorted(((fz, fy, fx) for fz in range(2) for fy in range(2) for fx in range(2) if fz or fy or fx),
               key=lambda s: -sum(s))


COMBINE_ORDER = tuple(16 * z + 4 * y + x for o in (0, 7, 1, 2, 4, 3, 5, 6)
                      for z in (o // 4 * 2, o // 4 * 2 + 1) for y in (o // 2 % 2 * 2, o // 2 % 2 * 2 + 1)
                      for x in (o % 2 * 2, o % 2 * 2 + 1))


def slot_of(sp):
    z, y, x = sp // 16, sp // 4 % 4, sp % 4
    return 32 * (z // 2) + 4 * (z % 2) + 16 * (y // 2) + 2 * (y % 2) + 8 * (x // 2) + x % 2


def kernel(seq_hbm, x_hbm, lnw_hbm, wq_hbm, wo_hbm, wg_hbm, wu_hbm, wd_hbm, k_hbm, v_hbm, out_ref,
           seq_ref, x_v, lnw_v, h_v, wq_v, k_v, v_v, wg_v, wu_v, wd_v, wo_v, q_v, s_v, p_v, stat_v, lse_v,
           att_send, att_recv, mlp_send, mlp_recv, half_send, half_recv, sum_send, sum_recv, fin,
           x_sem, wq_sem, k_sem, v_sem, w_sem, send_sem, att_rs, mlp_rs, half_rs, sum_rs, fin_rs):
    n_rows, width = x_v.shape
    n_kv, seq_block, head_dim = k_v.shape[1:]
    n_heads = q_v.shape[0] // n_rows
    inner = wg_v.shape[1]
    o_rows = wo_v.shape[0]
    per_row = n_kv // 2
    piece = width // N_CHIPS
    piece_rows = piece // LANES
    tp = lax.axis_index('tp')
    sp = lax.axis_index('sp')
    z, y, x = lax.div(sp, 16), lax.rem(lax.div(sp, 4), 4), lax.rem(sp, 4)
    zs, ys, xs = ([lax.rem(c + d, SIDE) for d in range(SIDE)] for c in (z, y, x))
    mine = (32 * lax.div(z, 2) + 4 * lax.rem(z, 2) + 16 * lax.div(y, 2) + 2 * lax.rem(y, 2)
            + 8 * lax.div(x, 2) + lax.rem(x, 2))
    row, corner = lax.div(mine, N_CHIPS), lax.rem(mine, N_CHIPS)
    at_z, at_y = [16 * c for c in zs], [4 * c for c in ys]
    flip_z, flip_y, flip_x = ([c, c + 1 - 2 * lax.rem(c, 2)] for c in (z, y, x))

    def step_to(s):
        return at_z[s[0]] + at_y[s[1]] + xs[s[2]]

    def in_order(order):
        for to in order[:-1]:
            is_me = sp == to
            yield jnp.where(is_me, order[-1], to), jnp.where(is_me, slot_of(order[-1]), slot_of(to))

    def flip_to(f):
        return 16 * flip_z[f[0]] + 4 * flip_y[f[1]] + flip_x[f[2]]

    q_starts = [sum(Q_CHUNKS[:i]) for i in range(len(Q_CHUNKS))]
    v_starts = [sum(V_GROUPS[:i]) for i in range(len(V_GROUPS))]

    def wq_copy(i):
        at = pl.ds(q_starts[i], Q_CHUNKS[i])
        return pltpu.make_async_copy(wq_hbm.at[at], wq_v.at[at], wq_sem.at[i])

    def k_copy(i):
        at = pl.ds(i * (n_rows // 2), n_rows // 2)
        return pltpu.make_async_copy(k_hbm.at[at], k_v.at[at], k_sem.at[i])

    def v_copy(i):
        at = pl.ds(v_starts[i], V_GROUPS[i])
        return pltpu.make_async_copy(v_hbm.at[at], v_v.at[at], v_sem.at[i])

    quarter = 2 * lax.div(z, 2) + lax.div(y, 2)
    shares_mlp = quarter < 3
    share = lax.rem(16 * quarter + 8 * lax.rem(z, 2) + 4 * lax.rem(y, 2) + x, N_INNER)
    inner_at = pl.multiple_of(share * inner, LANES)
    wg_copy = pltpu.make_async_copy(wg_hbm.at[:, pl.ds(inner_at, inner)], wg_v, w_sem.at[0])
    wu_copy = pltpu.make_async_copy(wu_hbm.at[:, pl.ds(inner_at, inner)], wu_v, w_sem.at[1])
    wd_copy = pltpu.make_async_copy(wd_hbm.at[pl.ds(inner_at, inner)], wd_v, w_sem.at[2])
    wo_copy = pltpu.make_async_copy(wo_hbm.at[pl.ds(pl.multiple_of(corner * o_rows, o_rows), o_rows)], wo_v, w_sem.at[3])
    x_copy = pltpu.make_async_copy(x_hbm, x_v, x_sem.at[0])
    lnw_copy = pltpu.make_async_copy(lnw_hbm, lnw_v, x_sem.at[1])
    seq_copy = pltpu.make_async_copy(seq_hbm, seq_ref, x_sem.at[2])

    with jax.named_scope('entry'):
        barrier = pltpu.get_barrier_semaphore()

        def tell(to_tp, to_sp):
            pl.semaphore_signal(barrier, inc=1, device_id={'tp': to_tp, 'sp': to_sp}, device_id_type=MESH)

        x_copy.start()
        lnw_copy.start()
        tell(1 - tp, sp)
        for i in range(len(Q_CHUNKS)):
            wq_copy(i).start()
        seq_copy.start()
        for s in STEPS[:32]:
            tell(tp, step_to(s))
        k_copy(0).start()
        k_copy(1).start()
        for s in STEPS[32:]:
            tell(tp, step_to(s))
        for i in range(len(V_GROUPS)):
            v_copy(i).start()
        for f in FLIPS:
            tell(1 - tp, flip_to(f))
        wg_copy.start()
        wu_copy.start()

    with jax.named_scope('wait_x'):
        x_copy.wait()
    with jax.named_scope('wait_lnw'):
        lnw_copy.wait()
    with jax.named_scope('norm'):
        x_f32 = x_v[...].astype(jnp.float32)
        centered = x_f32 - jnp.mean(x_f32, axis=-1, keepdims=True)
        variance = jnp.mean(centered * centered, axis=-1, keepdims=True)
        scale = lnw_v[...].astype(jnp.float32).reshape(1, width)
        h_v[...] = (centered * lax.rsqrt(variance + LN_EPS) * scale).astype(jnp.bfloat16)

    with jax.named_scope('query'):
        query = jnp.zeros((n_rows, n_heads * head_dim), jnp.float32)
        for i in range(len(Q_CHUNKS)):
            wq_copy(i).wait()
            at = slice(q_starts[i], q_starts[i] + Q_CHUNKS[i])
            query += jnp.dot(h_v[:, at], wq_v[at, :], preferred_element_type=jnp.float32)
        query = query.astype(jnp.bfloat16).astype(jnp.float32)
        for h in range(n_heads):
            q_v[h * n_rows:(h + 1) * n_rows, :] = query[:, h * head_dim:(h + 1) * head_dim]

    low_lanes = lax.broadcasted_iota(jnp.int32, (1, head_dim), 1) < head_dim // 2
    first_kv = lax.broadcasted_iota(jnp.int32, (8, head_dim), 0) < 4
    positions = sp * seq_block + lax.broadcasted_iota(jnp.int32, (8, seq_block), 1)

    def score(b, j):
        at = pl.ds((b * per_row + j) * 8, 8)
        q8 = q_v[pl.ds(j * 8 * n_rows + b, 8, stride=n_rows), :]
        zero = jnp.zeros_like(q8)
        q_wide = jnp.concatenate([jnp.where(first_kv, q8, zero), jnp.where(first_kv, zero, q8)], axis=1)
        k_wide = jnp.concatenate([k_v[b, 2 * j], k_v[b, 2 * j + 1]], axis=1)
        s_v[at, :] = lax.dot_general(q_wide.astype(jnp.bfloat16), k_wide, (((1,), (1,)), ((), ())),
                                     preferred_element_type=jnp.float32)

    def soften(b, j):
        at = pl.ds((b * per_row + j) * 8, 8)
        is_live = positions <= seq_ref[b]
        scores = jnp.where(is_live, s_v[at, :] * head_dim ** -0.5, NEG_BIG)
        block_max = jnp.max(scores, axis=-1, keepdims=True)
        probs = jnp.where(is_live, jnp.exp(scores - block_max), 0.0)
        block_sum = jnp.sum(probs, axis=-1, keepdims=True)
        p_v[at, :] = probs
        any_live = block_sum > 0.0
        safe_sum = jnp.where(any_live, block_sum, 1.0)
        lse_v[at, :] = jnp.broadcast_to(jnp.where(any_live, block_max + jnp.log(safe_sum), NEG_BIG), (8, head_dim))
        stat_v[at, :] = jnp.broadcast_to(1.0 / safe_sum, (8, head_dim))

    def value(b, j):
        at = pl.ds((b * per_row + j) * 8, 8)
        v_wide = jnp.concatenate([v_v[b, 2 * j], v_v[b, 2 * j + 1]], axis=1)
        wide = jnp.dot(p_v[at, :].astype(jnp.bfloat16), v_wide, preferred_element_type=jnp.float32)
        o8 = jnp.where(first_kv, wide[:, :head_dim], wide[:, head_dim:]) * stat_v[at, :]
        lse8 = lse_v[at, :]
        for r in range(4):
            att_send[b * 8 + j * 4 + r, 0:2, :] = o8[2 * r:2 * r + 2]
            att_send[b * 8 + j * 4 + r, 2:3, :] = jnp.where(low_lanes, lse8[2 * r:2 * r + 1], lse8[2 * r + 1:2 * r + 2])

    def sets(start, n):
        return [(b, j) for b in range(start, start + n) for j in range(per_row)]

    with jax.named_scope('scores'):
        wd_copy.start()
        wo_copy.start()
        seq_copy.wait()
        k_copy(0).wait()
        for c in sets(0, n_rows // 2):
            score(*c)
        k_copy(1).wait()
        for c in sets(n_rows // 2, n_rows // 2):
            score(*c)
        for c in sets(0, n_rows // 2):
            soften(*c)
    with jax.named_scope('values'):
        for i in range(len(V_GROUPS)):
            v_copy(i).wait()
            if i == 0:
                for c in sets(n_rows // 2, n_rows // 2):
                    soften(*c)
            for c in sets(v_starts[i], V_GROUPS[i]):
                value(*c)

    with jax.named_scope('att_send'):
        pl.semaphore_wait(barrier, N_SP - 1 + N_CHIPS)
        for to, slot in in_order(COMBINE_ORDER):
            pltpu.make_async_remote_copy(
                src_ref=att_send.at[slot, pl.ds(0, 3)], dst_ref=att_recv.at[sp, pl.ds(0, 3)],
                send_sem=send_sem.at[0], recv_sem=att_rs,
                device_id={'tp': tp, 'sp': to}, device_id_type=MESH).start()
        att_recv[sp] = att_send[mine]

    with jax.named_scope('mlp'):
        wg_copy.wait()
        wu_copy.wait()
        wd_copy.wait()

        @pl.when(shares_mlp)
        def _():
            up_wide = jnp.concatenate([wg_v[...], wu_v[...]], axis=1)
            wide = jnp.dot(h_v[...], up_wide, preferred_element_type=jnp.float32)
            gate, up = wide[:, :inner], wide[:, inner:]
            act = (gate * jax.nn.sigmoid(gate) * up).astype(jnp.bfloat16)
            for c in range(N_CHIPS):
                part = jnp.dot(act, wd_v[:, c * piece:(c + 1) * piece], preferred_element_type=jnp.float32)
                for b in range(n_rows):
                    for r in range(piece_rows):
                        mlp_send[b * N_CHIPS + c, r:r + 1, :] = part[b:b + 1, r * LANES:(r + 1) * LANES]

    with jax.named_scope('mlp_send'):
        @pl.when(shares_mlp)
        def _():
            for to, slot in in_order(COMBINE_ORDER):
                pltpu.make_async_remote_copy(
                    src_ref=mlp_send.at[slot], dst_ref=mlp_recv.at[share], send_sem=send_sem.at[1], recv_sem=mlp_rs,
                    device_id={'tp': tp, 'sp': to}, device_id_type=MESH).start()
            mlp_recv[share] = mlp_send[mine]

        wo_copy.wait()

    others = att_recv.at[pl.ds(0, N_SP - 1), pl.ds(0, 3)]
    with jax.named_scope('att_wait'):
        pltpu.make_async_copy(others, others, att_rs).wait()
    with jax.named_scope('combine'):
        lse = att_recv[:, 2, :]
        weight = jnp.exp(lse - jnp.max(lse, axis=0, keepdims=True))
        swapped = pltpu.roll(weight, head_dim // 2, 1)
        attn = []
        for h in range(2):
            spread = jnp.where(low_lanes, weight, swapped) if h == 0 else jnp.where(low_lanes, swapped, weight)
            attn.append(jnp.sum(att_recv[:, h, :] * spread, axis=0, keepdims=True)
                        / jnp.sum(spread, axis=0, keepdims=True))
        attn = jnp.concatenate(attn, axis=1)
        is_row = lax.broadcasted_iota(jnp.int32, (n_rows, 2 * head_dim), 0) == row
        attn = jnp.where(is_row, jnp.broadcast_to(attn, is_row.shape), 0.0).astype(jnp.bfloat16)
        is_mine = lax.broadcasted_iota(jnp.int32, (n_rows, piece), 0) == row
    with jax.named_scope('out_proj'):
        member = corner * 2 + tp
        flips = FLIPS + [(0, 0, 0)]
        pieces_of = [4 * lax.rem(flip_z[f[0]], 2) + 2 * lax.rem(flip_y[f[1]], 2) + lax.rem(flip_x[f[2]], 2) for f in flips]
        for i in range(0, N_CHIPS, 4):
            for c in pieces_of[i:i + 4]:
                at = pl.ds(pl.multiple_of(c * piece, piece), piece)
                total = jnp.dot(attn, wo_v[:, at], preferred_element_type=jnp.float32)
                total = jnp.sum(jnp.where(is_mine, total, 0.0), axis=0, keepdims=True)
                for r in range(piece_rows):
                    sum_send[c, r:r + 1, :] = total[:, r * LANES:(r + 1) * LANES]
            for f, c in zip(flips[i:i + 4], pieces_of[i:i + 4]):
                for ptp in ((tp, 1 - tp) if any(f) else (1 - tp,)):
                    pltpu.make_async_remote_copy(
                        src_ref=sum_send.at[c], dst_ref=sum_recv.at[member], send_sem=send_sem.at[2], recv_sem=sum_rs,
                        device_id={'tp': ptp, 'sp': flip_to(f)}, device_id_type=MESH).start()
        sum_recv[member] = sum_send[corner]

    with jax.named_scope('mlp_wait'):
        for is_sender in (True, False):
            @pl.when(shares_mlp == is_sender)
            def _():
                heard = mlp_recv.at[pl.ds(0, N_INNER - is_sender)]
                pltpu.make_async_copy(heard, heard, mlp_rs).wait()

    with jax.named_scope('half_send'):
        half_send[...] = jnp.sum(mlp_recv[...], axis=0)
        half_copy = pltpu.make_async_remote_copy(
            src_ref=half_send, dst_ref=half_recv, send_sem=send_sem.at[2], recv_sem=half_rs,
            device_id={'tp': 1 - tp, 'sp': sp}, device_id_type=MESH)
        half_copy.start()
    pieces = sum_recv.at[pl.ds(0, N_GROUP - 1)]
    with jax.named_scope('sum_wait'):
        pltpu.make_async_copy(pieces, pieces, sum_rs).wait()
    with jax.named_scope('half_wait'):
        half_copy.wait_recv()

    with jax.named_scope('fin_send'):
        fin[mine] = jnp.sum(sum_recv[...], axis=0) + (half_send[...] + half_recv[...])
        for to, _ in in_order(FINISH_ORDER):
            pltpu.make_async_remote_copy(
                src_ref=fin.at[mine], dst_ref=fin.at[mine], send_sem=send_sem.at[3], recv_sem=fin_rs,
                device_id={'tp': tp, 'sp': to}, device_id_type=MESH).start()
    arrived = fin.at[pl.ds(0, N_SP - 1)]
    with jax.named_scope('fin_wait'):
        pltpu.make_async_copy(arrived, arrived, fin_rs).wait()
    with jax.named_scope('finish'):
        for c in range(width // LANES):
            m, r = c // piece_rows, c % piece_rows
            rows = jnp.concatenate([fin[b * N_CHIPS + m, r:r + 1, :] for b in range(n_rows)], axis=0)
            at = slice(c * LANES, (c + 1) * LANES)
            out_ref[:, at] = (x_v[:, at].astype(jnp.float32) + rows).astype(jnp.bfloat16)
    with jax.named_scope('drain'):
        pltpu.make_async_copy(others, others, send_sem.at[0]).wait()

        @pl.when(shares_mlp)
        def _():
            sent = mlp_send.at[pl.ds(0, N_SP - 1)]
            pltpu.make_async_copy(sent, sent, send_sem.at[1]).wait()

        both = fin.at[pl.ds(0, N_GROUP)]
        pltpu.make_async_copy(both, both, send_sem.at[2]).wait()
        pltpu.make_async_copy(arrived, arrived, send_sem.at[3]).wait()


def solution(mesh):
    cache_spec = P(None, 'tp', 'sp', None)
    col_spec = P(None, 'tp')
    row_spec = P('tp', None)

    def local_step(x, seq_len, ln_w, w_q, w_o, w_gate, w_up, w_down, k_cache, v_cache):
        n_rows, n_kv, seq_block, head_dim = k_cache.shape
        width = x.shape[1]
        q_width = w_q.shape[1]
        inner = w_gate.shape[1] // N_INNER
        piece_rows = width // N_CHIPS // LANES
        n_queries = n_rows * q_width // head_dim
        hbm = pl.BlockSpec(memory_space=pltpu.HBM)
        dma = pltpu.SemaphoreType.DMA
        return pl.pallas_call(
            kernel,
            out_shape=jax.ShapeDtypeStruct((n_rows, width), jnp.bfloat16),
            in_specs=[hbm] * 10,
            out_specs=pl.BlockSpec(memory_space=pltpu.VMEM),
            scratch_shapes=[
                pltpu.SMEM((n_rows,), jnp.int32),
                pltpu.VMEM((n_rows, width), jnp.bfloat16),
                pltpu.VMEM((width,), jnp.bfloat16),
                pltpu.VMEM((n_rows, width), jnp.bfloat16),
                pltpu.VMEM((width, q_width), jnp.bfloat16),
                pltpu.VMEM(k_cache.shape, jnp.bfloat16),
                pltpu.VMEM(v_cache.shape, jnp.bfloat16),
                pltpu.VMEM((width, inner), jnp.bfloat16),
                pltpu.VMEM((width, inner), jnp.bfloat16),
                pltpu.VMEM((inner, width), jnp.bfloat16),
                pltpu.VMEM((q_width // N_CHIPS, width), jnp.bfloat16),
                pltpu.VMEM((n_queries, head_dim), jnp.float32),
                pltpu.VMEM((n_queries, seq_block), jnp.float32),
                pltpu.VMEM((n_queries, seq_block), jnp.float32),
                pltpu.VMEM((n_queries, head_dim), jnp.float32),
                pltpu.VMEM((n_queries, head_dim), jnp.float32),
                pltpu.VMEM((N_SP, 4, LANES), jnp.float32),
                pltpu.VMEM((N_SP, 4, LANES), jnp.float32),
                pltpu.VMEM((N_SP, piece_rows, LANES), jnp.float32),
                pltpu.VMEM((N_INNER, piece_rows, LANES), jnp.float32),
                pltpu.VMEM((piece_rows, LANES), jnp.float32),
                pltpu.VMEM((piece_rows, LANES), jnp.float32),
                pltpu.VMEM((N_CHIPS, piece_rows, LANES), jnp.float32),
                pltpu.VMEM((N_GROUP, piece_rows, LANES), jnp.float32),
                pltpu.VMEM((N_SP, piece_rows, LANES), jnp.float32),
                dma((3,)), dma((len(Q_CHUNKS),)), dma((2,)), dma((len(V_GROUPS),)), dma((4,)),
                dma((4,)), dma, dma, dma, dma, dma,
            ],
            compiler_params=pltpu.CompilerParams(
                collective_id=0, has_side_effects=True, vmem_limit_bytes=40 * 1024 * 1024),
        )(*(pltpu.with_memory_space_constraint(a, pltpu.HBM)
            for a in (seq_len, x, ln_w, w_q, w_o, w_gate, w_up, w_down, k_cache, v_cache)))

    return jax.shard_map(local_step, mesh=mesh,
                         in_specs=(P(), P(), P(), col_spec, row_spec,
                                   col_spec, col_spec, row_spec, cache_spec, cache_spec),
                         out_specs=P(), check_vma=False)
```

```python
import jax
import jax.numpy as jnp
from jax import lax
from jax.experimental import pallas as pl
from jax.experimental.pallas import tpu as pltpu
from jax.sharding import PartitionSpec as P

LN_EPS = 1e-5
NEG_BIG = -1e30
MESH = pl.DeviceIdType.MESH
SIDE = 4
N_SP = SIDE ** 3
N_CHIPS = 8
N_GROUP = 2 * N_CHIPS
LANES = 128
Q_CHUNKS = (1024, 1024, 1024, 512, 256, 256)
V_GROUPS = (4, 3, 1)
N_INNER = 48


def hops(d):
    return min(d, SIDE - d)


STEPS = sorted(((dz, dy, dx) for dz in range(SIDE) for dy in range(SIDE) for dx in range(SIDE) if dz or dy or dx),
               key=lambda s: -sum(hops(d) for d in s))
FINISH_ORDER = (
    0, 3, 12, 4, 1, 16, 2, 8, 15, 48, 7, 32, 19, 11, 13, 28,
    14, 5, 20, 51, 17, 6, 35, 60, 9, 44, 18, 24, 31, 10, 52, 49,
    23, 36, 50, 33, 56, 63, 34, 29, 40, 47, 27, 21, 30, 55, 22, 39,
    61, 25, 59, 45, 53, 62, 26, 43, 46, 37, 54, 38, 57, 41, 58, 42,
)
FLIPS = sorted(((fz, fy, fx) for fz in range(2) for fy in range(2) for fx in range(2) if fz or fy or fx),
               key=lambda s: -sum(s))


COMBINE_ORDER = tuple(16 * z + 4 * y + x for o in (0, 7, 1, 2, 4, 3, 5, 6)
                      for z in (o // 4 * 2, o // 4 * 2 + 1) for y in (o // 2 % 2 * 2, o // 2 % 2 * 2 + 1)
                      for x in (o % 2 * 2, o % 2 * 2 + 1))


def slot_of(sp):
    z, y, x = sp // 16, sp // 4 % 4, sp % 4
    return 32 * (z // 2) + 4 * (z % 2) + 16 * (y // 2) + 2 * (y % 2) + 8 * (x // 2) + x % 2


def kernel(seq_hbm, x_hbm, lnw_hbm, wq_hbm, wo_hbm, wg_hbm, wu_hbm, wd_hbm, k_hbm, v_hbm, out_ref,
           seq_ref, x_v, lnw_v, h_v, wq_v, k_v, v_v, wg_v, wu_v, wd_v, wo_v, q_v, s_v, p_v, stat_v, lse_v,
           att_send, att_recv, mlp_send, mlp_recv, half_send, half_recv, sum_send, sum_recv, fin,
           x_sem, wq_sem, k_sem, v_sem, w_sem, send_sem, att_rs, mlp_rs, half_rs, sum_rs, fin_rs):
    n_rows, width = x_v.shape
    n_kv, seq_block, head_dim = k_v.shape[1:]
    n_heads = q_v.shape[0] // n_rows
    inner = wg_v.shape[1]
    o_rows = wo_v.shape[0]
    per_row = n_kv // 2
    piece = width // N_CHIPS
    piece_rows = piece // LANES
    tp = lax.axis_index('tp')
    sp = lax.axis_index('sp')
    z, y, x = lax.div(sp, 16), lax.rem(lax.div(sp, 4), 4), lax.rem(sp, 4)
    zs, ys, xs = ([lax.rem(c + d, SIDE) for d in range(SIDE)] for c in (z, y, x))
    mine = (32 * lax.div(z, 2) + 4 * lax.rem(z, 2) + 16 * lax.div(y, 2) + 2 * lax.rem(y, 2)
            + 8 * lax.div(x, 2) + lax.rem(x, 2))
    row, corner = lax.div(mine, N_CHIPS), lax.rem(mine, N_CHIPS)
    at_z, at_y = [16 * c for c in zs], [4 * c for c in ys]
    flip_z, flip_y, flip_x = ([c, c + 1 - 2 * lax.rem(c, 2)] for c in (z, y, x))

    def step_to(s):
        return at_z[s[0]] + at_y[s[1]] + xs[s[2]]

    def in_order(order):
        for to in order[:-1]:
            is_me = sp == to
            yield jnp.where(is_me, order[-1], to), jnp.where(is_me, slot_of(order[-1]), slot_of(to))

    def flip_to(f):
        return 16 * flip_z[f[0]] + 4 * flip_y[f[1]] + flip_x[f[2]]

    q_starts = [sum(Q_CHUNKS[:i]) for i in range(len(Q_CHUNKS))]
    v_starts = [sum(V_GROUPS[:i]) for i in range(len(V_GROUPS))]

    def wq_copy(i):
        at = pl.ds(q_starts[i], Q_CHUNKS[i])
        return pltpu.make_async_copy(wq_hbm.at[at], wq_v.at[at], wq_sem.at[i])

    def k_copy(i):
        at = pl.ds(i * (n_rows // 2), n_rows // 2)
        return pltpu.make_async_copy(k_hbm.at[at], k_v.at[at], k_sem.at[i])

    def v_copy(i):
        at = pl.ds(v_starts[i], V_GROUPS[i])
        return pltpu.make_async_copy(v_hbm.at[at], v_v.at[at], v_sem.at[i])

    quarter = 2 * lax.div(z, 2) + lax.div(y, 2)
    shares_mlp = quarter < 3
    share = lax.rem(16 * quarter + 8 * lax.rem(z, 2) + 4 * lax.rem(y, 2) + x, N_INNER)
    inner_at = pl.multiple_of(share * inner, LANES)
    wg_copy = pltpu.make_async_copy(wg_hbm.at[:, pl.ds(inner_at, inner)], wg_v, w_sem.at[0])
    wu_copy = pltpu.make_async_copy(wu_hbm.at[:, pl.ds(inner_at, inner)], wu_v, w_sem.at[1])
    wd_copy = pltpu.make_async_copy(wd_hbm.at[pl.ds(inner_at, inner)], wd_v, w_sem.at[2])
    wo_copy = pltpu.make_async_copy(wo_hbm.at[pl.ds(pl.multiple_of(corner * o_rows, o_rows), o_rows)], wo_v, w_sem.at[3])
    x_copy = pltpu.make_async_copy(x_hbm, x_v, x_sem.at[0])
    lnw_copy = pltpu.make_async_copy(lnw_hbm, lnw_v, x_sem.at[1])
    seq_copy = pltpu.make_async_copy(seq_hbm, seq_ref, x_sem.at[2])

    with jax.named_scope('entry'):
        barrier = pltpu.get_barrier_semaphore()

        def tell(to_tp, to_sp):
            pl.semaphore_signal(barrier, inc=1, device_id={'tp': to_tp, 'sp': to_sp}, device_id_type=MESH)

        x_copy.start()
        lnw_copy.start()
        tell(1 - tp, sp)
        for i in range(len(Q_CHUNKS)):
            wq_copy(i).start()
        seq_copy.start()
        for s in STEPS[:32]:
            tell(tp, step_to(s))
        k_copy(0).start()
        k_copy(1).start()
        for s in STEPS[32:]:
            tell(tp, step_to(s))
        for i in range(len(V_GROUPS)):
            v_copy(i).start()
        for f in FLIPS:
            tell(1 - tp, flip_to(f))
        wg_copy.start()
        wu_copy.start()

    with jax.named_scope('wait_x'):
        x_copy.wait()
    with jax.named_scope('wait_lnw'):
        lnw_copy.wait()
    with jax.named_scope('norm'):
        x_f32 = x_v[...].astype(jnp.float32)
        centered = x_f32 - jnp.mean(x_f32, axis=-1, keepdims=True)
        variance = jnp.mean(centered * centered, axis=-1, keepdims=True)
        scale = lnw_v[...].astype(jnp.float32).reshape(1, width)
        h_v[...] = (centered * lax.rsqrt(variance + LN_EPS) * scale).astype(jnp.bfloat16)

    with jax.named_scope('query'):
        query = jnp.zeros((n_rows, n_heads * head_dim), jnp.float32)
        for i in range(len(Q_CHUNKS)):
            wq_copy(i).wait()
            at = slice(q_starts[i], q_starts[i] + Q_CHUNKS[i])
            query += jnp.dot(h_v[:, at], wq_v[at, :], preferred_element_type=jnp.float32)
        query = query.astype(jnp.bfloat16).astype(jnp.float32)
        for h in range(n_heads):
            q_v[h * n_rows:(h + 1) * n_rows, :] = query[:, h * head_dim:(h + 1) * head_dim]

    low_lanes = lax.broadcasted_iota(jnp.int32, (1, head_dim), 1) < head_dim // 2
    first_kv = lax.broadcasted_iota(jnp.int32, (8, head_dim), 0) < 4
    positions = sp * seq_block + lax.broadcasted_iota(jnp.int32, (8, seq_block), 1)

    def score(b, j):
        at = pl.ds((b * per_row + j) * 8, 8)
        q8 = q_v[pl.ds(j * 8 * n_rows + b, 8, stride=n_rows), :]
        zero = jnp.zeros_like(q8)
        q_wide = jnp.concatenate([jnp.where(first_kv, q8, zero), jnp.where(first_kv, zero, q8)], axis=1)
        k_wide = jnp.concatenate([k_v[b, 2 * j], k_v[b, 2 * j + 1]], axis=1)
        s_v[at, :] = lax.dot_general(q_wide.astype(jnp.bfloat16), k_wide, (((1,), (1,)), ((), ())),
                                     preferred_element_type=jnp.float32)

    def soften(b, j):
        at = pl.ds((b * per_row + j) * 8, 8)
        is_live = positions <= seq_ref[b]
        scores = jnp.where(is_live, s_v[at, :] * head_dim ** -0.5, NEG_BIG)
        block_max = jnp.max(scores, axis=-1, keepdims=True)
        probs = jnp.where(is_live, jnp.exp(scores - block_max), 0.0)
        block_sum = jnp.sum(probs, axis=-1, keepdims=True)
        p_v[at, :] = probs
        any_live = block_sum > 0.0
        safe_sum = jnp.where(any_live, block_sum, 1.0)
        lse_v[at, :] = jnp.broadcast_to(jnp.where(any_live, block_max + jnp.log(safe_sum), NEG_BIG), (8, head_dim))
        stat_v[at, :] = jnp.broadcast_to(1.0 / safe_sum, (8, head_dim))

    def value(b, j):
        at = pl.ds((b * per_row + j) * 8, 8)
        v_wide = jnp.concatenate([v_v[b, 2 * j], v_v[b, 2 * j + 1]], axis=1)
        wide = jnp.dot(p_v[at, :].astype(jnp.bfloat16), v_wide, preferred_element_type=jnp.float32)
        o8 = jnp.where(first_kv, wide[:, :head_dim], wide[:, head_dim:]) * stat_v[at, :]
        lse8 = lse_v[at, :]
        for r in range(4):
            att_send[b * 8 + j * 4 + r, 0:2, :] = o8[2 * r:2 * r + 2]
            att_send[b * 8 + j * 4 + r, 2:3, :] = jnp.where(low_lanes, lse8[2 * r:2 * r + 1], lse8[2 * r + 1:2 * r + 2])

    def sets(start, n):
        return [(b, j) for b in range(start, start + n) for j in range(per_row)]

    with jax.named_scope('scores'):
        wd_copy.start()
        wo_copy.start()
        seq_copy.wait()
        k_copy(0).wait()
        for c in sets(0, n_rows // 2):
            score(*c)
        k_copy(1).wait()
        for c in sets(n_rows // 2, n_rows // 2):
            score(*c)
        for c in sets(0, n_rows // 2):
            soften(*c)
    with jax.named_scope('values'):
        for i in range(len(V_GROUPS)):
            v_copy(i).wait()
            if i == 0:
                for c in sets(n_rows // 2, n_rows // 2):
                    soften(*c)
            for c in sets(v_starts[i], V_GROUPS[i]):
                value(*c)

    with jax.named_scope('att_send'):
        pl.semaphore_wait(barrier, N_SP - 1 + N_CHIPS)
        for to, slot in in_order(COMBINE_ORDER):
            pltpu.make_async_remote_copy(
                src_ref=att_send.at[slot, pl.ds(0, 3)], dst_ref=att_recv.at[sp, pl.ds(0, 3)],
                send_sem=send_sem.at[0], recv_sem=att_rs,
                device_id={'tp': tp, 'sp': to}, device_id_type=MESH).start()
        att_recv[sp] = att_send[mine]

    with jax.named_scope('mlp'):
        wg_copy.wait()
        wu_copy.wait()
        wd_copy.wait()

        @pl.when(shares_mlp)
        def _():
            up_wide = jnp.concatenate([wg_v[...], wu_v[...]], axis=1)
            wide = jnp.dot(h_v[...], up_wide, preferred_element_type=jnp.float32)
            gate, up = wide[:, :inner], wide[:, inner:]
            act = (gate * jax.nn.sigmoid(gate) * up).astype(jnp.bfloat16)
            for c in range(N_CHIPS):
                part = jnp.dot(act, wd_v[:, c * piece:(c + 1) * piece], preferred_element_type=jnp.float32)
                for b in range(n_rows):
                    for r in range(piece_rows):
                        mlp_send[b * N_CHIPS + c, r:r + 1, :] = part[b:b + 1, r * LANES:(r + 1) * LANES]

    with jax.named_scope('mlp_send'):
        @pl.when(shares_mlp)
        def _():
            for to, slot in in_order(COMBINE_ORDER):
                pltpu.make_async_remote_copy(
                    src_ref=mlp_send.at[slot], dst_ref=mlp_recv.at[share], send_sem=send_sem.at[1], recv_sem=mlp_rs,
                    device_id={'tp': tp, 'sp': to}, device_id_type=MESH).start()
            mlp_recv[share] = mlp_send[mine]

        wo_copy.wait()

    others = att_recv.at[pl.ds(0, N_SP - 1), pl.ds(0, 3)]
    with jax.named_scope('att_wait'):
        pltpu.make_async_copy(others, others, att_rs).wait()
    with jax.named_scope('combine'):
        lse = att_recv[:, 2, :]
        weight = jnp.exp(lse - jnp.max(lse, axis=0, keepdims=True))
        swapped = pltpu.roll(weight, head_dim // 2, 1)
        attn = []
        for h in range(2):
            spread = jnp.where(low_lanes, weight, swapped) if h == 0 else jnp.where(low_lanes, swapped, weight)
            attn.append(jnp.sum(att_recv[:, h, :] * spread, axis=0, keepdims=True)
                        / jnp.sum(spread, axis=0, keepdims=True))
        attn = jnp.concatenate(attn, axis=1)
        is_row = lax.broadcasted_iota(jnp.int32, (n_rows, 2 * head_dim), 0) == row
        attn = jnp.where(is_row, jnp.broadcast_to(attn, is_row.shape), 0.0).astype(jnp.bfloat16)
        is_mine = lax.broadcasted_iota(jnp.int32, (n_rows, width), 0) == row
    with jax.named_scope('out_proj'):
        member = corner * 2 + tp
        flips = FLIPS + [(0, 0, 0)]
        pieces_of = [4 * lax.rem(flip_z[f[0]], 2) + 2 * lax.rem(flip_y[f[1]], 2) + lax.rem(flip_x[f[2]], 2) for f in flips]
        total = jnp.dot(attn, wo_v[...], preferred_element_type=jnp.float32)
        total = jnp.sum(jnp.where(is_mine, total, 0.0), axis=0, keepdims=True)
        for k in range(width // LANES):
            c, r = k // piece_rows, k % piece_rows
            sum_send[c, r:r + 1, :] = total[:, k * LANES:(k + 1) * LANES]
        for f, c in zip(flips, pieces_of):
            for ptp in ((tp, 1 - tp) if any(f) else (1 - tp,)):
                pltpu.make_async_remote_copy(
                    src_ref=sum_send.at[c], dst_ref=sum_recv.at[member], send_sem=send_sem.at[2], recv_sem=sum_rs,
                    device_id={'tp': ptp, 'sp': flip_to(f)}, device_id_type=MESH).start()
        sum_recv[member] = sum_send[corner]

    with jax.named_scope('mlp_wait'):
        for is_sender in (True, False):
            @pl.when(shares_mlp == is_sender)
            def _():
                heard = mlp_recv.at[pl.ds(0, N_INNER - is_sender)]
                pltpu.make_async_copy(heard, heard, mlp_rs).wait()

    with jax.named_scope('half_send'):
        half_send[...] = jnp.sum(mlp_recv[...], axis=0)
        half_copy = pltpu.make_async_remote_copy(
            src_ref=half_send, dst_ref=half_recv, send_sem=send_sem.at[2], recv_sem=half_rs,
            device_id={'tp': 1 - tp, 'sp': sp}, device_id_type=MESH)
        half_copy.start()
    pieces = sum_recv.at[pl.ds(0, N_GROUP - 1)]
    with jax.named_scope('sum_wait'):
        pltpu.make_async_copy(pieces, pieces, sum_rs).wait()
    with jax.named_scope('half_wait'):
        half_copy.wait_recv()

    with jax.named_scope('fin_send'):
        fin[mine] = jnp.sum(sum_recv[...], axis=0) + (half_send[...] + half_recv[...])
        for to, _ in in_order(FINISH_ORDER):
            pltpu.make_async_remote_copy(
                src_ref=fin.at[mine], dst_ref=fin.at[mine], send_sem=send_sem.at[3], recv_sem=fin_rs,
                device_id={'tp': tp, 'sp': to}, device_id_type=MESH).start()
    arrived = fin.at[pl.ds(0, N_SP - 1)]
    with jax.named_scope('fin_wait'):
        pltpu.make_async_copy(arrived, arrived, fin_rs).wait()
    with jax.named_scope('finish'):
        for c in range(width // LANES):
            m, r = c // piece_rows, c % piece_rows
            rows = jnp.concatenate([fin[b * N_CHIPS + m, r:r + 1, :] for b in range(n_rows)], axis=0)
            at = slice(c * LANES, (c + 1) * LANES)
            out_ref[:, at] = (x_v[:, at].astype(jnp.float32) + rows).astype(jnp.bfloat16)
    with jax.named_scope('drain'):
        pltpu.make_async_copy(others, others, send_sem.at[0]).wait()

        @pl.when(shares_mlp)
        def _():
            sent = mlp_send.at[pl.ds(0, N_SP - 1)]
            pltpu.make_async_copy(sent, sent, send_sem.at[1]).wait()

        both = fin.at[pl.ds(0, N_GROUP)]
        pltpu.make_async_copy(both, both, send_sem.at[2]).wait()
        pltpu.make_async_copy(arrived, arrived, send_sem.at[3]).wait()


def solution(mesh):
    cache_spec = P(None, 'tp', 'sp', None)
    col_spec = P(None, 'tp')
    row_spec = P('tp', None)

    def local_step(x, seq_len, ln_w, w_q, w_o, w_gate, w_up, w_down, k_cache, v_cache):
        n_rows, n_kv, seq_block, head_dim = k_cache.shape
        width = x.shape[1]
        q_width = w_q.shape[1]
        inner = w_gate.shape[1] // N_INNER
        piece_rows = width // N_CHIPS // LANES
        n_queries = n_rows * q_width // head_dim
        hbm = pl.BlockSpec(memory_space=pltpu.HBM)
        dma = pltpu.SemaphoreType.DMA
        return pl.pallas_call(
            kernel,
            out_shape=jax.ShapeDtypeStruct((n_rows, width), jnp.bfloat16),
            in_specs=[hbm] * 10,
            out_specs=pl.BlockSpec(memory_space=pltpu.VMEM),
            scratch_shapes=[
                pltpu.SMEM((n_rows,), jnp.int32),
                pltpu.VMEM((n_rows, width), jnp.bfloat16),
                pltpu.VMEM((width,), jnp.bfloat16),
                pltpu.VMEM((n_rows, width), jnp.bfloat16),
                pltpu.VMEM((width, q_width), jnp.bfloat16),
                pltpu.VMEM(k_cache.shape, jnp.bfloat16),
                pltpu.VMEM(v_cache.shape, jnp.bfloat16),
                pltpu.VMEM((width, inner), jnp.bfloat16),
                pltpu.VMEM((width, inner), jnp.bfloat16),
                pltpu.VMEM((inner, width), jnp.bfloat16),
                pltpu.VMEM((q_width // N_CHIPS, width), jnp.bfloat16),
                pltpu.VMEM((n_queries, head_dim), jnp.float32),
                pltpu.VMEM((n_queries, seq_block), jnp.float32),
                pltpu.VMEM((n_queries, seq_block), jnp.float32),
                pltpu.VMEM((n_queries, head_dim), jnp.float32),
                pltpu.VMEM((n_queries, head_dim), jnp.float32),
                pltpu.VMEM((N_SP, 4, LANES), jnp.float32),
                pltpu.VMEM((N_SP, 4, LANES), jnp.float32),
                pltpu.VMEM((N_SP, piece_rows, LANES), jnp.float32),
                pltpu.VMEM((N_INNER, piece_rows, LANES), jnp.float32),
                pltpu.VMEM((piece_rows, LANES), jnp.float32),
                pltpu.VMEM((piece_rows, LANES), jnp.float32),
                pltpu.VMEM((N_CHIPS, piece_rows, LANES), jnp.float32),
                pltpu.VMEM((N_GROUP, piece_rows, LANES), jnp.float32),
                pltpu.VMEM((N_SP, piece_rows, LANES), jnp.float32),
                dma((3,)), dma((len(Q_CHUNKS),)), dma((2,)), dma((len(V_GROUPS),)), dma((4,)),
                dma((4,)), dma, dma, dma, dma, dma,
            ],
            compiler_params=pltpu.CompilerParams(
                collective_id=0, has_side_effects=True, vmem_limit_bytes=40 * 1024 * 1024),
        )(*(pltpu.with_memory_space_constraint(a, pltpu.HBM)
            for a in (seq_len, x, ln_w, w_q, w_o, w_gate, w_up, w_down, k_cache, v_cache)))

    return jax.shard_map(local_step, mesh=mesh,
                         in_specs=(P(), P(), P(), col_spec, row_spec,
                                   col_spec, col_spec, row_spec, cache_spec, cache_spec),
                         out_specs=P(), check_vma=False)
```

```python
import jax
import jax.numpy as jnp
from jax import lax
from jax.experimental import pallas as pl
from jax.experimental.pallas import tpu as pltpu
from jax.sharding import PartitionSpec as P

LN_EPS = 1e-5
NEG_BIG = -1e30
MESH = pl.DeviceIdType.MESH
SIDE = 4
N_SP = SIDE ** 3
N_CHIPS = 8
N_GROUP = 2 * N_CHIPS
LANES = 128
Q_CHUNKS = (1024, 1024, 1024, 512, 256, 256)
V_GROUPS = (4, 3, 1)
N_INNER = 48


def hops(d):
    return min(d, SIDE - d)


STEPS = sorted(((dz, dy, dx) for dz in range(SIDE) for dy in range(SIDE) for dx in range(SIDE) if dz or dy or dx),
               key=lambda s: -sum(hops(d) for d in s))
FINISH_ORDER = (
    0, 12, 3, 1, 4, 16, 2, 57, 54, 8, 48, 35, 6, 19, 34, 36,
    40, 7, 49, 42, 15, 56, 31, 25, 62, 37, 41, 14, 59, 28, 45, 11,
    22, 32, 47, 58, 23, 44, 20, 60, 24, 51, 17, 46, 5, 43, 38, 9,
    18, 52, 21, 53, 63, 29, 30, 26, 33, 61, 27, 10, 55, 39, 50, 13,
)
FLIPS = sorted(((fz, fy, fx) for fz in range(2) for fy in range(2) for fx in range(2) if fz or fy or fx),
               key=lambda s: -sum(s))


COMBINE_ORDER = (
    0, 32, 8, 40, 34, 10, 2, 42, 6, 38, 4, 36, 46, 9, 63, 56,
    24, 33, 43, 41, 1, 26, 37, 7, 16, 53, 5, 39, 35, 29, 11, 3,
    14, 51, 58, 52, 47, 60, 49, 44, 57, 50, 61, 45, 12, 17, 15, 27,
    19, 48, 20, 25, 55, 22, 30, 21, 31, 59, 13, 54, 23, 62, 28, 18,
)


def slot_of(sp):
    z, y, x = sp // 16, sp // 4 % 4, sp % 4
    return 32 * (z // 2) + 4 * (z % 2) + 16 * (y // 2) + 2 * (y % 2) + 8 * (x // 2) + x % 2


def kernel(seq_hbm, x_hbm, lnw_hbm, wq_hbm, wo_hbm, wg_hbm, wu_hbm, wd_hbm, k_hbm, v_hbm, out_ref,
           seq_ref, x_v, lnw_v, h_v, wq_v, k_v, v_v, wg_v, wu_v, wd_v, wo_v, q_v, s_v, p_v, stat_v, lse_v,
           att_send, att_recv, mlp_send, mlp_recv, half_send, half_recv, sum_send, sum_recv, fin,
           x_sem, wq_sem, k_sem, v_sem, w_sem, send_sem, att_rs, mlp_rs, half_rs, sum_rs, fin_rs):
    n_rows, width = x_v.shape
    n_kv, seq_block, head_dim = k_v.shape[1:]
    n_heads = q_v.shape[0] // n_rows
    inner = wg_v.shape[1]
    o_rows = wo_v.shape[0]
    per_row = n_kv // 2
    piece = width // N_CHIPS
    piece_rows = piece // LANES
    tp = lax.axis_index('tp')
    sp = lax.axis_index('sp')
    z, y, x = lax.div(sp, 16), lax.rem(lax.div(sp, 4), 4), lax.rem(sp, 4)
    zs, ys, xs = ([lax.rem(c + d, SIDE) for d in range(SIDE)] for c in (z, y, x))
    mine = (32 * lax.div(z, 2) + 4 * lax.rem(z, 2) + 16 * lax.div(y, 2) + 2 * lax.rem(y, 2)
            + 8 * lax.div(x, 2) + lax.rem(x, 2))
    row, corner = lax.div(mine, N_CHIPS), lax.rem(mine, N_CHIPS)
    at_z, at_y = [16 * c for c in zs], [4 * c for c in ys]
    flip_z, flip_y, flip_x = ([c, c + 1 - 2 * lax.rem(c, 2)] for c in (z, y, x))

    def step_to(s):
        return at_z[s[0]] + at_y[s[1]] + xs[s[2]]

    def in_order(order):
        for to in order[:-1]:
            is_me = sp == to
            yield jnp.where(is_me, order[-1], to), jnp.where(is_me, slot_of(order[-1]), slot_of(to))

    def flip_to(f):
        return 16 * flip_z[f[0]] + 4 * flip_y[f[1]] + flip_x[f[2]]

    q_starts = [sum(Q_CHUNKS[:i]) for i in range(len(Q_CHUNKS))]
    v_starts = [sum(V_GROUPS[:i]) for i in range(len(V_GROUPS))]

    def wq_copy(i):
        at = pl.ds(q_starts[i], Q_CHUNKS[i])
        return pltpu.make_async_copy(wq_hbm.at[at], wq_v.at[at], wq_sem.at[i])

    def k_copy(i):
        at = pl.ds(i * (n_rows // 2), n_rows // 2)
        return pltpu.make_async_copy(k_hbm.at[at], k_v.at[at], k_sem.at[i])

    def v_copy(i):
        at = pl.ds(v_starts[i], V_GROUPS[i])
        return pltpu.make_async_copy(v_hbm.at[at], v_v.at[at], v_sem.at[i])

    quarter = 2 * lax.div(z, 2) + lax.div(y, 2)
    shares_mlp = quarter < 3
    share = lax.rem(16 * quarter + 8 * lax.rem(z, 2) + 4 * lax.rem(y, 2) + x, N_INNER)
    inner_at = pl.multiple_of(share * inner, LANES)
    wg_copy = pltpu.make_async_copy(wg_hbm.at[:, pl.ds(inner_at, inner)], wg_v, w_sem.at[0])
    wu_copy = pltpu.make_async_copy(wu_hbm.at[:, pl.ds(inner_at, inner)], wu_v, w_sem.at[1])
    wd_copy = pltpu.make_async_copy(wd_hbm.at[pl.ds(inner_at, inner)], wd_v, w_sem.at[2])
    wo_copy = pltpu.make_async_copy(wo_hbm.at[pl.ds(pl.multiple_of(corner * o_rows, o_rows), o_rows)], wo_v, w_sem.at[3])
    x_copy = pltpu.make_async_copy(x_hbm, x_v, x_sem.at[0])
    lnw_copy = pltpu.make_async_copy(lnw_hbm, lnw_v, x_sem.at[1])
    seq_copy = pltpu.make_async_copy(seq_hbm, seq_ref, x_sem.at[2])

    with jax.named_scope('entry'):
        barrier = pltpu.get_barrier_semaphore()

        def tell(to_tp, to_sp):
            pl.semaphore_signal(barrier, inc=1, device_id={'tp': to_tp, 'sp': to_sp}, device_id_type=MESH)

        x_copy.start()
        lnw_copy.start()
        tell(1 - tp, sp)
        for i in range(len(Q_CHUNKS)):
            wq_copy(i).start()
        seq_copy.start()
        for s in STEPS[:32]:
            tell(tp, step_to(s))
        k_copy(0).start()
        k_copy(1).start()
        for s in STEPS[32:]:
            tell(tp, step_to(s))
        for i in range(len(V_GROUPS)):
            v_copy(i).start()
        for f in FLIPS:
            tell(1 - tp, flip_to(f))
        wg_copy.start()
        wu_copy.start()

    with jax.named_scope('wait_x'):
        x_copy.wait()
    with jax.named_scope('wait_lnw'):
        lnw_copy.wait()
    with jax.named_scope('norm'):
        x_f32 = x_v[...].astype(jnp.float32)
        centered = x_f32 - jnp.mean(x_f32, axis=-1, keepdims=True)
        variance = jnp.mean(centered * centered, axis=-1, keepdims=True)
        scale = lnw_v[...].astype(jnp.float32).reshape(1, width)
        h_v[...] = (centered * lax.rsqrt(variance + LN_EPS) * scale).astype(jnp.bfloat16)

    with jax.named_scope('query'):
        query = jnp.zeros((n_rows, n_heads * head_dim), jnp.float32)
        for i in range(len(Q_CHUNKS)):
            wq_copy(i).wait()
            at = slice(q_starts[i], q_starts[i] + Q_CHUNKS[i])
            query += jnp.dot(h_v[:, at], wq_v[at, :], preferred_element_type=jnp.float32)
        query = query.astype(jnp.bfloat16).astype(jnp.float32)
        for h in range(n_heads):
            q_v[h * n_rows:(h + 1) * n_rows, :] = query[:, h * head_dim:(h + 1) * head_dim]

    low_lanes = lax.broadcasted_iota(jnp.int32, (1, head_dim), 1) < head_dim // 2
    first_kv = lax.broadcasted_iota(jnp.int32, (8, head_dim), 0) < 4
    positions = sp * seq_block + lax.broadcasted_iota(jnp.int32, (8, seq_block), 1)

    def score(b, j):
        at = pl.ds((b * per_row + j) * 8, 8)
        q8 = q_v[pl.ds(j * 8 * n_rows + b, 8, stride=n_rows), :]
        zero = jnp.zeros_like(q8)
        q_wide = jnp.concatenate([jnp.where(first_kv, q8, zero), jnp.where(first_kv, zero, q8)], axis=1)
        k_wide = jnp.concatenate([k_v[b, 2 * j], k_v[b, 2 * j + 1]], axis=1)
        s_v[at, :] = lax.dot_general(q_wide.astype(jnp.bfloat16), k_wide, (((1,), (1,)), ((), ())),
                                     preferred_element_type=jnp.float32)

    def soften(b, j):
        at = pl.ds((b * per_row + j) * 8, 8)
        is_live = positions <= seq_ref[b]
        scores = jnp.where(is_live, s_v[at, :] * head_dim ** -0.5, NEG_BIG)
        block_max = jnp.max(scores, axis=-1, keepdims=True)
        probs = jnp.where(is_live, jnp.exp(scores - block_max), 0.0)
        block_sum = jnp.sum(probs, axis=-1, keepdims=True)
        p_v[at, :] = probs
        any_live = block_sum > 0.0
        safe_sum = jnp.where(any_live, block_sum, 1.0)
        lse_v[at, :] = jnp.broadcast_to(jnp.where(any_live, block_max + jnp.log(safe_sum), NEG_BIG), (8, head_dim))
        stat_v[at, :] = jnp.broadcast_to(1.0 / safe_sum, (8, head_dim))

    def value(b, j):
        at = pl.ds((b * per_row + j) * 8, 8)
        v_wide = jnp.concatenate([v_v[b, 2 * j], v_v[b, 2 * j + 1]], axis=1)
        wide = jnp.dot(p_v[at, :].astype(jnp.bfloat16), v_wide, preferred_element_type=jnp.float32)
        o8 = jnp.where(first_kv, wide[:, :head_dim], wide[:, head_dim:]) * stat_v[at, :]
        lse8 = lse_v[at, :]
        for r in range(4):
            att_send[b * 8 + j * 4 + r, 0:2, :] = o8[2 * r:2 * r + 2]
            att_send[b * 8 + j * 4 + r, 2:3, :] = jnp.where(low_lanes, lse8[2 * r:2 * r + 1], lse8[2 * r + 1:2 * r + 2])

    def sets(start, n):
        return [(b, j) for b in range(start, start + n) for j in range(per_row)]

    with jax.named_scope('scores'):
        wd_copy.start()
        wo_copy.start()
        seq_copy.wait()
        k_copy(0).wait()
        for c in sets(0, n_rows // 2):
            score(*c)
        k_copy(1).wait()
        for c in sets(n_rows // 2, n_rows // 2):
            score(*c)
        for c in sets(0, n_rows // 2):
            soften(*c)
    with jax.named_scope('values'):
        for i in range(len(V_GROUPS)):
            v_copy(i).wait()
            if i == 0:
                for c in sets(n_rows // 2, n_rows // 2):
                    soften(*c)
            for c in sets(v_starts[i], V_GROUPS[i]):
                value(*c)

    with jax.named_scope('att_send'):
        pl.semaphore_wait(barrier, N_SP - 1 + N_CHIPS)
        for to, slot in in_order(COMBINE_ORDER):
            pltpu.make_async_remote_copy(
                src_ref=att_send.at[slot, pl.ds(0, 3)], dst_ref=att_recv.at[sp, pl.ds(0, 3)],
                send_sem=send_sem.at[0], recv_sem=att_rs,
                device_id={'tp': tp, 'sp': to}, device_id_type=MESH).start()
        att_recv[sp] = att_send[mine]

    with jax.named_scope('mlp'):
        wg_copy.wait()
        wu_copy.wait()
        wd_copy.wait()

        @pl.when(shares_mlp)
        def _():
            up_wide = jnp.concatenate([wg_v[...], wu_v[...]], axis=1)
            wide = jnp.dot(h_v[...], up_wide, preferred_element_type=jnp.float32)
            gate, up = wide[:, :inner], wide[:, inner:]
            act = (gate * jax.nn.sigmoid(gate) * up).astype(jnp.bfloat16)
            for c in range(N_CHIPS):
                part = jnp.dot(act, wd_v[:, c * piece:(c + 1) * piece], preferred_element_type=jnp.float32)
                for b in range(n_rows):
                    for r in range(piece_rows):
                        mlp_send[b * N_CHIPS + c, r:r + 1, :] = part[b:b + 1, r * LANES:(r + 1) * LANES]

    with jax.named_scope('mlp_send'):
        @pl.when(shares_mlp)
        def _():
            for to, slot in in_order(COMBINE_ORDER):
                pltpu.make_async_remote_copy(
                    src_ref=mlp_send.at[slot], dst_ref=mlp_recv.at[share], send_sem=send_sem.at[1], recv_sem=mlp_rs,
                    device_id={'tp': tp, 'sp': to}, device_id_type=MESH).start()
            mlp_recv[share] = mlp_send[mine]

        wo_copy.wait()

    others = att_recv.at[pl.ds(0, N_SP - 1), pl.ds(0, 3)]
    with jax.named_scope('att_wait'):
        pltpu.make_async_copy(others, others, att_rs).wait()
    with jax.named_scope('combine'):
        lse = att_recv[:, 2, :]
        weight = jnp.exp(lse - jnp.max(lse, axis=0, keepdims=True))
        swapped = pltpu.roll(weight, head_dim // 2, 1)
        attn = []
        for h in range(2):
            spread = jnp.where(low_lanes, weight, swapped) if h == 0 else jnp.where(low_lanes, swapped, weight)
            attn.append(jnp.sum(att_recv[:, h, :] * spread, axis=0, keepdims=True)
                        / jnp.sum(spread, axis=0, keepdims=True))
        attn = jnp.concatenate(attn, axis=1)
        is_row = lax.broadcasted_iota(jnp.int32, (n_rows, 2 * head_dim), 0) == row
        attn = jnp.where(is_row, jnp.broadcast_to(attn, is_row.shape), 0.0).astype(jnp.bfloat16)
        is_mine = lax.broadcasted_iota(jnp.int32, (n_rows, piece), 0) == row
    with jax.named_scope('out_proj'):
        member = corner * 2 + tp
        flips = FLIPS + [(0, 0, 0)]
        pieces_of = [4 * lax.rem(flip_z[f[0]], 2) + 2 * lax.rem(flip_y[f[1]], 2) + lax.rem(flip_x[f[2]], 2) for f in flips]
        for i in range(0, N_CHIPS, 4):
            for c in pieces_of[i:i + 4]:
                at = pl.ds(pl.multiple_of(c * piece, piece), piece)
                total = jnp.dot(attn, wo_v[:, at], preferred_element_type=jnp.float32)
                total = jnp.sum(jnp.where(is_mine, total, 0.0), axis=0, keepdims=True)
                for r in range(piece_rows):
                    sum_send[c, r:r + 1, :] = total[:, r * LANES:(r + 1) * LANES]
            for f, c in zip(flips[i:i + 4], pieces_of[i:i + 4]):
                for ptp in ((tp, 1 - tp) if any(f) else (1 - tp,)):
                    pltpu.make_async_remote_copy(
                        src_ref=sum_send.at[c], dst_ref=sum_recv.at[member], send_sem=send_sem.at[2], recv_sem=sum_rs,
                        device_id={'tp': ptp, 'sp': flip_to(f)}, device_id_type=MESH).start()
        sum_recv[member] = sum_send[corner]

    with jax.named_scope('mlp_wait'):
        for is_sender in (True, False):
            @pl.when(shares_mlp == is_sender)
            def _():
                heard = mlp_recv.at[pl.ds(0, N_INNER - is_sender)]
                pltpu.make_async_copy(heard, heard, mlp_rs).wait()

    with jax.named_scope('half_send'):
        half_send[...] = jnp.sum(mlp_recv[...], axis=0)
        half_copy = pltpu.make_async_remote_copy(
            src_ref=half_send, dst_ref=half_recv, send_sem=send_sem.at[2], recv_sem=half_rs,
            device_id={'tp': 1 - tp, 'sp': sp}, device_id_type=MESH)
        half_copy.start()
    pieces = sum_recv.at[pl.ds(0, N_GROUP - 1)]
    with jax.named_scope('sum_wait'):
        pltpu.make_async_copy(pieces, pieces, sum_rs).wait()
    with jax.named_scope('half_wait'):
        half_copy.wait_recv()

    with jax.named_scope('fin_send'):
        fin[mine] = jnp.sum(sum_recv[...], axis=0) + (half_send[...] + half_recv[...])
        for to, _ in in_order(FINISH_ORDER):
            pltpu.make_async_remote_copy(
                src_ref=fin.at[mine], dst_ref=fin.at[mine], send_sem=send_sem.at[3], recv_sem=fin_rs,
                device_id={'tp': tp, 'sp': to}, device_id_type=MESH).start()
    arrived = fin.at[pl.ds(0, N_SP - 1)]
    with jax.named_scope('fin_wait'):
        pltpu.make_async_copy(arrived, arrived, fin_rs).wait()
    with jax.named_scope('finish'):
        for c in range(width // LANES):
            m, r = c // piece_rows, c % piece_rows
            rows = jnp.concatenate([fin[b * N_CHIPS + m, r:r + 1, :] for b in range(n_rows)], axis=0)
            at = slice(c * LANES, (c + 1) * LANES)
            out_ref[:, at] = (x_v[:, at].astype(jnp.float32) + rows).astype(jnp.bfloat16)
    with jax.named_scope('drain'):
        pltpu.make_async_copy(others, others, send_sem.at[0]).wait()

        @pl.when(shares_mlp)
        def _():
            sent = mlp_send.at[pl.ds(0, N_SP - 1)]
            pltpu.make_async_copy(sent, sent, send_sem.at[1]).wait()

        both = fin.at[pl.ds(0, N_GROUP)]
        pltpu.make_async_copy(both, both, send_sem.at[2]).wait()
        pltpu.make_async_copy(arrived, arrived, send_sem.at[3]).wait()


def solution(mesh):
    cache_spec = P(None, 'tp', 'sp', None)
    col_spec = P(None, 'tp')
    row_spec = P('tp', None)

    def local_step(x, seq_len, ln_w, w_q, w_o, w_gate, w_up, w_down, k_cache, v_cache):
        n_rows, n_kv, seq_block, head_dim = k_cache.shape
        width = x.shape[1]
        q_width = w_q.shape[1]
        inner = w_gate.shape[1] // N_INNER
        piece_rows = width // N_CHIPS // LANES
        n_queries = n_rows * q_width // head_dim
        hbm = pl.BlockSpec(memory_space=pltpu.HBM)
        dma = pltpu.SemaphoreType.DMA
        return pl.pallas_call(
            kernel,
            out_shape=jax.ShapeDtypeStruct((n_rows, width), jnp.bfloat16),
            in_specs=[hbm] * 10,
            out_specs=pl.BlockSpec(memory_space=pltpu.VMEM),
            scratch_shapes=[
                pltpu.SMEM((n_rows,), jnp.int32),
                pltpu.VMEM((n_rows, width), jnp.bfloat16),
                pltpu.VMEM((width,), jnp.bfloat16),
                pltpu.VMEM((n_rows, width), jnp.bfloat16),
                pltpu.VMEM((width, q_width), jnp.bfloat16),
                pltpu.VMEM(k_cache.shape, jnp.bfloat16),
                pltpu.VMEM(v_cache.shape, jnp.bfloat16),
                pltpu.VMEM((width, inner), jnp.bfloat16),
                pltpu.VMEM((width, inner), jnp.bfloat16),
                pltpu.VMEM((inner, width), jnp.bfloat16),
                pltpu.VMEM((q_width // N_CHIPS, width), jnp.bfloat16),
                pltpu.VMEM((n_queries, head_dim), jnp.float32),
                pltpu.VMEM((n_queries, seq_block), jnp.float32),
                pltpu.VMEM((n_queries, seq_block), jnp.float32),
                pltpu.VMEM((n_queries, head_dim), jnp.float32),
                pltpu.VMEM((n_queries, head_dim), jnp.float32),
                pltpu.VMEM((N_SP, 4, LANES), jnp.float32),
                pltpu.VMEM((N_SP, 4, LANES), jnp.float32),
                pltpu.VMEM((N_SP, piece_rows, LANES), jnp.float32),
                pltpu.VMEM((N_INNER, piece_rows, LANES), jnp.float32),
                pltpu.VMEM((piece_rows, LANES), jnp.float32),
                pltpu.VMEM((piece_rows, LANES), jnp.float32),
                pltpu.VMEM((N_CHIPS, piece_rows, LANES), jnp.float32),
                pltpu.VMEM((N_GROUP, piece_rows, LANES), jnp.float32),
                pltpu.VMEM((N_SP, piece_rows, LANES), jnp.float32),
                dma((3,)), dma((len(Q_CHUNKS),)), dma((2,)), dma((len(V_GROUPS),)), dma((4,)),
                dma((4,)), dma, dma, dma, dma, dma,
            ],
            compiler_params=pltpu.CompilerParams(
                collective_id=0, has_side_effects=True, vmem_limit_bytes=40 * 1024 * 1024),
        )(*(pltpu.with_memory_space_constraint(a, pltpu.HBM)
            for a in (seq_len, x, ln_w, w_q, w_o, w_gate, w_up, w_down, k_cache, v_cache)))

    return jax.shard_map(local_step, mesh=mesh,
                         in_specs=(P(), P(), P(), col_spec, row_spec,
                                   col_spec, col_spec, row_spec, cache_spec, cache_spec),
                         out_specs=P(), check_vma=False)
```

```python
import jax
import jax.numpy as jnp
from jax import lax
from jax.experimental import pallas as pl
from jax.experimental.pallas import tpu as pltpu
from jax.sharding import PartitionSpec as P

LN_EPS = 1e-5
NEG_BIG = -1e30
MESH = pl.DeviceIdType.MESH
SIDE = 4
N_SP = SIDE ** 3
N_CHIPS = 8
N_GROUP = 2 * N_CHIPS
LANES = 128
Q_CHUNKS = (1024, 1024, 1024, 512, 256, 256)
V_GROUPS = (4, 3, 1)
N_INNER = 48


def hops(d):
    return min(d, SIDE - d)


STEPS = sorted(((dz, dy, dx) for dz in range(SIDE) for dy in range(SIDE) for dx in range(SIDE) if dz or dy or dx),
               key=lambda s: -sum(hops(d) for d in s))
FINISH_STEPS = sorted(STEPS, key=lambda s: -sum((0.0, 1.37, 0.84, 0.42)[d] for d in s))
FLIPS = sorted(((fz, fy, fx) for fz in range(2) for fy in range(2) for fx in range(2) if fz or fy or fx),
               key=lambda s: -sum(s))


COMBINE_ORDER = (
    0, 32, 8, 40, 34, 10, 2, 42, 6, 38, 4, 36, 46, 9, 63, 56,
    24, 33, 43, 41, 1, 26, 37, 7, 16, 53, 5, 39, 35, 29, 11, 3,
    14, 51, 58, 52, 47, 60, 49, 44, 57, 50, 61, 45, 12, 17, 15, 27,
    19, 48, 20, 25, 55, 22, 30, 21, 31, 59, 13, 54, 23, 62, 28, 18,
)


def slot_of(sp):
    z, y, x = sp // 16, sp // 4 % 4, sp % 4
    return 32 * (z // 2) + 4 * (z % 2) + 16 * (y // 2) + 2 * (y % 2) + 8 * (x // 2) + x % 2


def kernel(seq_hbm, x_hbm, lnw_hbm, wq_hbm, wo_hbm, wg_hbm, wu_hbm, wd_hbm, k_hbm, v_hbm, out_ref,
           seq_ref, x_v, lnw_v, h_v, wq_v, k_v, v_v, wg_v, wu_v, wd_v, wo_v, q_v, s_v, p_v, stat_v, lse_v,
           att_send, att_recv, mlp_send, mlp_recv, half_send, half_recv, sum_send, sum_recv, fin,
           x_sem, wq_sem, k_sem, v_sem, w_sem, send_sem, att_rs, mlp_rs, half_rs, sum_rs, fin_rs):
    n_rows, width = x_v.shape
    n_kv, seq_block, head_dim = k_v.shape[1:]
    n_heads = q_v.shape[0] // n_rows
    inner = wg_v.shape[1]
    o_rows = wo_v.shape[0]
    per_row = n_kv // 2
    piece = width // N_CHIPS
    piece_rows = piece // LANES
    tp = lax.axis_index('tp')
    sp = lax.axis_index('sp')
    z, y, x = lax.div(sp, 16), lax.rem(lax.div(sp, 4), 4), lax.rem(sp, 4)
    zs, ys, xs = ([lax.rem(c + d, SIDE) for d in range(SIDE)] for c in (z, y, x))
    mine = (32 * lax.div(z, 2) + 4 * lax.rem(z, 2) + 16 * lax.div(y, 2) + 2 * lax.rem(y, 2)
            + 8 * lax.div(x, 2) + lax.rem(x, 2))
    row, corner = lax.div(mine, N_CHIPS), lax.rem(mine, N_CHIPS)
    at_z, at_y = [16 * c for c in zs], [4 * c for c in ys]
    flip_z, flip_y, flip_x = ([c, c + 1 - 2 * lax.rem(c, 2)] for c in (z, y, x))

    def step_to(s):
        return at_z[s[0]] + at_y[s[1]] + xs[s[2]]

    def in_order(order):
        for to in order[:-1]:
            is_me = sp == to
            yield jnp.where(is_me, order[-1], to), jnp.where(is_me, slot_of(order[-1]), slot_of(to))

    def flip_to(f):
        return 16 * flip_z[f[0]] + 4 * flip_y[f[1]] + flip_x[f[2]]

    q_starts = [sum(Q_CHUNKS[:i]) for i in range(len(Q_CHUNKS))]
    v_starts = [sum(V_GROUPS[:i]) for i in range(len(V_GROUPS))]

    def wq_copy(i):
        at = pl.ds(q_starts[i], Q_CHUNKS[i])
        return pltpu.make_async_copy(wq_hbm.at[at], wq_v.at[at], wq_sem.at[i])

    def k_copy(i):
        at = pl.ds(i * (n_rows // 2), n_rows // 2)
        return pltpu.make_async_copy(k_hbm.at[at], k_v.at[at], k_sem.at[i])

    def v_copy(i):
        at = pl.ds(v_starts[i], V_GROUPS[i])
        return pltpu.make_async_copy(v_hbm.at[at], v_v.at[at], v_sem.at[i])

    quarter = 2 * lax.div(z, 2) + lax.div(y, 2)
    shares_mlp = quarter < 3
    share = lax.rem(16 * quarter + 8 * lax.rem(z, 2) + 4 * lax.rem(y, 2) + x, N_INNER)
    inner_at = pl.multiple_of(share * inner, LANES)
    wg_copy = pltpu.make_async_copy(wg_hbm.at[:, pl.ds(inner_at, inner)], wg_v, w_sem.at[0])
    wu_copy = pltpu.make_async_copy(wu_hbm.at[:, pl.ds(inner_at, inner)], wu_v, w_sem.at[1])
    wd_copy = pltpu.make_async_copy(wd_hbm.at[pl.ds(inner_at, inner)], wd_v, w_sem.at[2])
    wo_copy = pltpu.make_async_copy(wo_hbm.at[pl.ds(pl.multiple_of(corner * o_rows, o_rows), o_rows)], wo_v, w_sem.at[3])
    x_copy = pltpu.make_async_copy(x_hbm, x_v, x_sem.at[0])
    lnw_copy = pltpu.make_async_copy(lnw_hbm, lnw_v, x_sem.at[1])
    seq_copy = pltpu.make_async_copy(seq_hbm, seq_ref, x_sem.at[2])

    with jax.named_scope('entry'):
        barrier = pltpu.get_barrier_semaphore()

        def tell(to_tp, to_sp):
            pl.semaphore_signal(barrier, inc=1, device_id={'tp': to_tp, 'sp': to_sp}, device_id_type=MESH)

        x_copy.start()
        lnw_copy.start()
        tell(1 - tp, sp)
        for i in range(len(Q_CHUNKS)):
            wq_copy(i).start()
        seq_copy.start()
        for s in STEPS[:32]:
            tell(tp, step_to(s))
        k_copy(0).start()
        k_copy(1).start()
        for s in STEPS[32:]:
            tell(tp, step_to(s))
        for i in range(len(V_GROUPS)):
            v_copy(i).start()
        for f in FLIPS:
            tell(1 - tp, flip_to(f))
        wg_copy.start()
        wu_copy.start()

    with jax.named_scope('wait_x'):
        x_copy.wait()
    with jax.named_scope('wait_lnw'):
        lnw_copy.wait()
    with jax.named_scope('norm'):
        x_f32 = x_v[...].astype(jnp.float32)
        centered = x_f32 - jnp.mean(x_f32, axis=-1, keepdims=True)
        variance = jnp.mean(centered * centered, axis=-1, keepdims=True)
        scale = lnw_v[...].astype(jnp.float32).reshape(1, width)
        h_v[...] = (centered * lax.rsqrt(variance + LN_EPS) * scale).astype(jnp.bfloat16)

    with jax.named_scope('query'):
        query = jnp.zeros((n_rows, n_heads * head_dim), jnp.float32)
        for i in range(len(Q_CHUNKS)):
            wq_copy(i).wait()
            at = slice(q_starts[i], q_starts[i] + Q_CHUNKS[i])
            query += jnp.dot(h_v[:, at], wq_v[at, :], preferred_element_type=jnp.float32)
        query = query.astype(jnp.bfloat16).astype(jnp.float32)
        for h in range(n_heads):
            q_v[h * n_rows:(h + 1) * n_rows, :] = query[:, h * head_dim:(h + 1) * head_dim]

    low_lanes = lax.broadcasted_iota(jnp.int32, (1, head_dim), 1) < head_dim // 2
    first_kv = lax.broadcasted_iota(jnp.int32, (8, head_dim), 0) < 4
    positions = sp * seq_block + lax.broadcasted_iota(jnp.int32, (8, seq_block), 1)

    def score(b, j):
        at = pl.ds((b * per_row + j) * 8, 8)
        q8 = q_v[pl.ds(j * 8 * n_rows + b, 8, stride=n_rows), :]
        zero = jnp.zeros_like(q8)
        q_wide = jnp.concatenate([jnp.where(first_kv, q8, zero), jnp.where(first_kv, zero, q8)], axis=1)
        k_wide = jnp.concatenate([k_v[b, 2 * j], k_v[b, 2 * j + 1]], axis=1)
        s_v[at, :] = lax.dot_general(q_wide.astype(jnp.bfloat16), k_wide, (((1,), (1,)), ((), ())),
                                     preferred_element_type=jnp.float32)

    def soften(b, j):
        at = pl.ds((b * per_row + j) * 8, 8)
        is_live = positions <= seq_ref[b]
        scores = jnp.where(is_live, s_v[at, :] * head_dim ** -0.5, NEG_BIG)
        block_max = jnp.max(scores, axis=-1, keepdims=True)
        probs = jnp.where(is_live, jnp.exp(scores - block_max), 0.0)
        block_sum = jnp.sum(probs, axis=-1, keepdims=True)
        p_v[at, :] = probs
        any_live = block_sum > 0.0
        safe_sum = jnp.where(any_live, block_sum, 1.0)
        lse_v[at, :] = jnp.broadcast_to(jnp.where(any_live, block_max + jnp.log(safe_sum), NEG_BIG), (8, head_dim))
        stat_v[at, :] = jnp.broadcast_to(1.0 / safe_sum, (8, head_dim))

    def value(b, j):
        at = pl.ds((b * per_row + j) * 8, 8)
        v_wide = jnp.concatenate([v_v[b, 2 * j], v_v[b, 2 * j + 1]], axis=1)
        wide = jnp.dot(p_v[at, :].astype(jnp.bfloat16), v_wide, preferred_element_type=jnp.float32)
        o8 = jnp.where(first_kv, wide[:, :head_dim], wide[:, head_dim:]) * stat_v[at, :]
        lse8 = lse_v[at, :]
        for r in range(4):
            att_send[b * 8 + j * 4 + r, 0:2, :] = o8[2 * r:2 * r + 2]
            att_send[b * 8 + j * 4 + r, 2:3, :] = jnp.where(low_lanes, lse8[2 * r:2 * r + 1], lse8[2 * r + 1:2 * r + 2])

    def sets(start, n):
        return [(b, j) for b in range(start, start + n) for j in range(per_row)]

    with jax.named_scope('scores'):
        wd_copy.start()
        wo_copy.start()
        seq_copy.wait()
        k_copy(0).wait()
        for c in sets(0, n_rows // 2):
            score(*c)
        k_copy(1).wait()
        for c in sets(n_rows // 2, n_rows // 2):
            score(*c)
        for c in sets(0, n_rows // 2):
            soften(*c)
    with jax.named_scope('values'):
        for i in range(len(V_GROUPS)):
            v_copy(i).wait()
            if i == 0:
                for c in sets(n_rows // 2, n_rows // 2):
                    soften(*c)
            for c in sets(v_starts[i], V_GROUPS[i]):
                value(*c)

    with jax.named_scope('att_send'):
        pl.semaphore_wait(barrier, N_SP - 1 + N_CHIPS)
        for to, slot in in_order(COMBINE_ORDER):
            pltpu.make_async_remote_copy(
                src_ref=att_send.at[slot, pl.ds(0, 3)], dst_ref=att_recv.at[sp, pl.ds(0, 3)],
                send_sem=send_sem.at[0], recv_sem=att_rs,
                device_id={'tp': tp, 'sp': to}, device_id_type=MESH).start()
        att_recv[sp] = att_send[mine]

    with jax.named_scope('mlp'):
        wg_copy.wait()
        wu_copy.wait()
        wd_copy.wait()

        @pl.when(shares_mlp)
        def _():
            up_wide = jnp.concatenate([wg_v[...], wu_v[...]], axis=1)
            wide = jnp.dot(h_v[...], up_wide, preferred_element_type=jnp.float32)
            gate, up = wide[:, :inner], wide[:, inner:]
            act = (gate * jax.nn.sigmoid(gate) * up).astype(jnp.bfloat16)
            for c in range(N_CHIPS):
                part = jnp.dot(act, wd_v[:, c * piece:(c + 1) * piece], preferred_element_type=jnp.float32)
                for b in range(n_rows):
                    for r in range(piece_rows):
                        mlp_send[b * N_CHIPS + c, r:r + 1, :] = part[b:b + 1, r * LANES:(r + 1) * LANES]

    with jax.named_scope('mlp_send'):
        @pl.when(shares_mlp)
        def _():
            for to, slot in in_order(COMBINE_ORDER):
                pltpu.make_async_remote_copy(
                    src_ref=mlp_send.at[slot], dst_ref=mlp_recv.at[share], send_sem=send_sem.at[1], recv_sem=mlp_rs,
                    device_id={'tp': tp, 'sp': to}, device_id_type=MESH).start()
            mlp_recv[share] = mlp_send[mine]

        wo_copy.wait()

    others = att_recv.at[pl.ds(0, N_SP - 1), pl.ds(0, 3)]
    with jax.named_scope('att_wait'):
        pltpu.make_async_copy(others, others, att_rs).wait()
    with jax.named_scope('combine'):
        lse = att_recv[:, 2, :]
        weight = jnp.exp(lse - jnp.max(lse, axis=0, keepdims=True))
        swapped = pltpu.roll(weight, head_dim // 2, 1)
        attn = []
        for h in range(2):
            spread = jnp.where(low_lanes, weight, swapped) if h == 0 else jnp.where(low_lanes, swapped, weight)
            attn.append(jnp.sum(att_recv[:, h, :] * spread, axis=0, keepdims=True)
                        / jnp.sum(spread, axis=0, keepdims=True))
        attn = jnp.concatenate(attn, axis=1)
        is_row = lax.broadcasted_iota(jnp.int32, (n_rows, 2 * head_dim), 0) == row
        attn = jnp.where(is_row, jnp.broadcast_to(attn, is_row.shape), 0.0).astype(jnp.bfloat16)
        is_mine = lax.broadcasted_iota(jnp.int32, (n_rows, piece), 0) == row
    with jax.named_scope('out_proj'):
        member = corner * 2 + tp
        flips = FLIPS + [(0, 0, 0)]
        pieces_of = [4 * lax.rem(flip_z[f[0]], 2) + 2 * lax.rem(flip_y[f[1]], 2) + lax.rem(flip_x[f[2]], 2) for f in flips]
        for i in range(0, N_CHIPS, 4):
            for c in pieces_of[i:i + 4]:
                at = pl.ds(pl.multiple_of(c * piece, piece), piece)
                total = jnp.dot(attn, wo_v[:, at], preferred_element_type=jnp.float32)
                total = jnp.sum(jnp.where(is_mine, total, 0.0), axis=0, keepdims=True)
                for r in range(piece_rows):
                    sum_send[c, r:r + 1, :] = total[:, r * LANES:(r + 1) * LANES]
            for f, c in zip(flips[i:i + 4], pieces_of[i:i + 4]):
                for ptp in ((tp, 1 - tp) if any(f) else (1 - tp,)):
                    pltpu.make_async_remote_copy(
                        src_ref=sum_send.at[c], dst_ref=sum_recv.at[member], send_sem=send_sem.at[2], recv_sem=sum_rs,
                        device_id={'tp': ptp, 'sp': flip_to(f)}, device_id_type=MESH).start()
        sum_recv[member] = sum_send[corner]

    with jax.named_scope('mlp_wait'):
        for is_sender in (True, False):
            @pl.when(shares_mlp == is_sender)
            def _():
                heard = mlp_recv.at[pl.ds(0, N_INNER - is_sender)]
                pltpu.make_async_copy(heard, heard, mlp_rs).wait()

    with jax.named_scope('half_send'):
        half_send[...] = jnp.sum(mlp_recv[...], axis=0)
        half_copy = pltpu.make_async_remote_copy(
            src_ref=half_send, dst_ref=half_recv, send_sem=send_sem.at[2], recv_sem=half_rs,
            device_id={'tp': 1 - tp, 'sp': sp}, device_id_type=MESH)
        half_copy.start()
    pieces = sum_recv.at[pl.ds(0, N_GROUP - 1)]
    with jax.named_scope('sum_wait'):
        pltpu.make_async_copy(pieces, pieces, sum_rs).wait()
    with jax.named_scope('half_wait'):
        half_copy.wait_recv()

    with jax.named_scope('fin_send'):
        fin[mine] = jnp.sum(sum_recv[...], axis=0) + (half_send[...] + half_recv[...])
        for s in FINISH_STEPS:
            pltpu.make_async_remote_copy(
                src_ref=fin.at[mine], dst_ref=fin.at[mine], send_sem=send_sem.at[3], recv_sem=fin_rs,
                device_id={'tp': tp, 'sp': step_to(s)}, device_id_type=MESH).start()
    arrived = fin.at[pl.ds(0, N_SP - 1)]
    with jax.named_scope('fin_wait'):
        pltpu.make_async_copy(arrived, arrived, fin_rs).wait()
    with jax.named_scope('finish'):
        for c in range(width // LANES):
            m, r = c // piece_rows, c % piece_rows
            rows = jnp.concatenate([fin[b * N_CHIPS + m, r:r + 1, :] for b in range(n_rows)], axis=0)
            at = slice(c * LANES, (c + 1) * LANES)
            out_ref[:, at] = (x_v[:, at].astype(jnp.float32) + rows).astype(jnp.bfloat16)
    with jax.named_scope('drain'):
        pltpu.make_async_copy(others, others, send_sem.at[0]).wait()

        @pl.when(shares_mlp)
        def _():
            sent = mlp_send.at[pl.ds(0, N_SP - 1)]
            pltpu.make_async_copy(sent, sent, send_sem.at[1]).wait()

        both = fin.at[pl.ds(0, N_GROUP)]
        pltpu.make_async_copy(both, both, send_sem.at[2]).wait()
        pltpu.make_async_copy(arrived, arrived, send_sem.at[3]).wait()


def solution(mesh):
    cache_spec = P(None, 'tp', 'sp', None)
    col_spec = P(None, 'tp')
    row_spec = P('tp', None)

    def local_step(x, seq_len, ln_w, w_q, w_o, w_gate, w_up, w_down, k_cache, v_cache):
        n_rows, n_kv, seq_block, head_dim = k_cache.shape
        width = x.shape[1]
        q_width = w_q.shape[1]
        inner = w_gate.shape[1] // N_INNER
        piece_rows = width // N_CHIPS // LANES
        n_queries = n_rows * q_width // head_dim
        hbm = pl.BlockSpec(memory_space=pltpu.HBM)
        dma = pltpu.SemaphoreType.DMA
        return pl.pallas_call(
            kernel,
            out_shape=jax.ShapeDtypeStruct((n_rows, width), jnp.bfloat16),
            in_specs=[hbm] * 10,
            out_specs=pl.BlockSpec(memory_space=pltpu.VMEM),
            scratch_shapes=[
                pltpu.SMEM((n_rows,), jnp.int32),
                pltpu.VMEM((n_rows, width), jnp.bfloat16),
                pltpu.VMEM((width,), jnp.bfloat16),
                pltpu.VMEM((n_rows, width), jnp.bfloat16),
                pltpu.VMEM((width, q_width), jnp.bfloat16),
                pltpu.VMEM(k_cache.shape, jnp.bfloat16),
                pltpu.VMEM(v_cache.shape, jnp.bfloat16),
                pltpu.VMEM((width, inner), jnp.bfloat16),
                pltpu.VMEM((width, inner), jnp.bfloat16),
                pltpu.VMEM((inner, width), jnp.bfloat16),
                pltpu.VMEM((q_width // N_CHIPS, width), jnp.bfloat16),
                pltpu.VMEM((n_queries, head_dim), jnp.float32),
                pltpu.VMEM((n_queries, seq_block), jnp.float32),
                pltpu.VMEM((n_queries, seq_block), jnp.float32),
                pltpu.VMEM((n_queries, head_dim), jnp.float32),
                pltpu.VMEM((n_queries, head_dim), jnp.float32),
                pltpu.VMEM((N_SP, 4, LANES), jnp.float32),
                pltpu.VMEM((N_SP, 4, LANES), jnp.float32),
                pltpu.VMEM((N_SP, piece_rows, LANES), jnp.float32),
                pltpu.VMEM((N_INNER, piece_rows, LANES), jnp.float32),
                pltpu.VMEM((piece_rows, LANES), jnp.float32),
                pltpu.VMEM((piece_rows, LANES), jnp.float32),
                pltpu.VMEM((N_CHIPS, piece_rows, LANES), jnp.float32),
                pltpu.VMEM((N_GROUP, piece_rows, LANES), jnp.float32),
                pltpu.VMEM((N_SP, piece_rows, LANES), jnp.float32),
                dma((3,)), dma((len(Q_CHUNKS),)), dma((2,)), dma((len(V_GROUPS),)), dma((4,)),
                dma((4,)), dma, dma, dma, dma, dma,
            ],
            compiler_params=pltpu.CompilerParams(
                collective_id=0, has_side_effects=True, vmem_limit_bytes=40 * 1024 * 1024),
        )(*(pltpu.with_memory_space_constraint(a, pltpu.HBM)
            for a in (seq_len, x, ln_w, w_q, w_o, w_gate, w_up, w_down, k_cache, v_cache)))

    return jax.shard_map(local_step, mesh=mesh,
                         in_specs=(P(), P(), P(), col_spec, row_spec,
                                   col_spec, col_spec, row_spec, cache_spec, cache_spec),
                         out_specs=P(), check_vma=False)
```
